128 devices in a mesh: dp: 32 (over y, z, core), mp: 4 (over x).
Axes of the slice: x: 4, y: 4, z: 4, core: 2. Of those that a mesh axis runs over, the one named last changes fastest.
Arguments:
- pred_input: bfloat16 [2048, 256, 384], P('dp'), may hold values from -6 to 6
- proj_weight: bfloat16 [384, 1280], P('dp', 'mp'), may hold values from -0.3125 to 0.3125
- proj_bias: float32 [1280], P('mp'), may hold values from -3 to 3
- targets: bfloat16 [2048, 256, 1280], P('dp', None, 'mp'), may hold values from -6 to 6
- block_masks: int32 [2048, 4, 256], P('dp'), may hold values from 0 to 1, as said below
Outputs:
- loss: float32 [], replicated
- clip_scale: float32 [], replicated
- grad_weight: float32 [384, 1280], P('dp', 'mp')
- grad_bias: float32 [1280], P('mp')
The draws below stay inside these ranges and needn't reach their ends.
Inputs may be any that keep to these rules, and one draw needn't show every extreme that they name: `block_masks`: each of an image's 4 target blocks is a nonempty rectangle of patches on the 16 x 16 grid (row-major patch order); blocks may intersect.
All inputs are finite; a program needn't handle non-finite values.
Results may differ from the reference program's by a relative error of at most 0.0003.
Values may be sent and summed in bfloat16 or wider, within the bound.
A program may use at most 192 MiB of HBM per device.

```python
import jax
import jax.numpy as jnp
from jax import lax

D = 1280
E = 384
GRID = 16
BLOCKS = 4
IMG_DEV = 64
PATCHES = 256
IMAGES = 2048


def draw_block_masks(key, part):
    keys = jax.random.split(key, 4)
    lowest = max(1, GRID * 5 // 16)
    highest = GRID // 2 + 1
    heights = jax.random.randint(keys[0], (IMAGES, BLOCKS, 1), lowest, highest)
    widths = jax.random.randint(keys[1], (IMAGES, BLOCKS, 1), lowest, highest)
    top_raw = jax.random.randint(keys[2], (IMAGES, BLOCKS, 1), 0, 1 << 20)
    left_raw = jax.random.randint(keys[3], (IMAGES, BLOCKS, 1), 0, 1 << 20)
    top_row = top_raw % (GRID - heights + 1)
    left_col = left_raw % (GRID - widths + 1)
    places = jnp.arange(GRID * GRID, dtype=jnp.int32)
    row_of = (places // GRID)[None, None, :]
    col_of = (places % GRID)[None, None, :]
    inside = (row_of >= top_row) & (row_of < top_row + heights) & (col_of >= left_col) & (col_of < left_col + widths)
    return inside.astype(jnp.int32)


def shard_levels(own_key, dims, pieces, low, high):
    level = 1.0
    for axis_at, blocks in pieces:
        draws = jax.random.uniform(jax.random.fold_in(jax.random.fold_in(own_key, 6), axis_at), (blocks,), jnp.float32, low / len(pieces), high / len(pieces))
        level = level * jnp.repeat(jnp.exp(draws), dims[axis_at] // blocks).reshape((-1,) + (1,) * (len(dims) - 1 - axis_at))
    return level


def scatter_about(rng, shape, spread, bound, pieces=(), held_as=jnp.bfloat16):
    values = spread * jax.random.normal(rng, shape, jnp.float32)
    if pieces:
        values = values * shard_levels(rng, shape, pieces, -0.22, 0.18)
    return jnp.clip(values, -bound, bound).astype(held_as)


def setup_inputs(seed: int = 0) -> dict:
    key_list = jax.random.split(jax.random.key(seed), 6)
    return {
        "pred_input": scatter_about(key_list[0], (IMAGES, PATCHES, E), 1.0, 6.0, ((0, 32),)),
        "proj_weight": scatter_about(key_list[1], (E, D), E ** -0.5, 0.3125, ((0, 32), (1, 4))),
        "proj_bias": scatter_about(key_list[2], (D,), 0.5, 3.0, ((0, 4),), jnp.float32),
        "targets": scatter_about(key_list[3], (IMAGES, PATCHES, D), 1.0, 6.0, ((0, 32), (2, 4))),
        "block_masks": draw_block_masks(jax.random.fold_in(key_list[5], 71), 0),
    }


def reference(pred_input, proj_weight, proj_bias, targets, block_masks):
    groups = IMAGES // IMG_DEV
    inputs_grouped = pred_input.reshape(groups, IMG_DEV * PATCHES, E)
    targets_grouped = targets.reshape(groups, IMG_DEV * PATCHES, D)
    coverage_all = lax.optimization_barrier(jnp.sum(block_masks, axis=1)).astype(jnp.float32)
    coverage_grouped = coverage_all.reshape(groups, IMG_DEV * PATCHES, 1)

    def step(carry, batch):
        grad_acc, bias_acc, loss_acc, count_acc = carry
        inputs_here, targets_here, coverage = batch
        target_f = targets_here.astype(jnp.float32)
        mean_feat = lax.optimization_barrier(jnp.mean(target_f, axis=1, keepdims=True))
        centered = target_f - mean_feat
        variance = lax.optimization_barrier(jnp.mean(centered * centered, axis=1, keepdims=True))
        tnorm = centered / jnp.sqrt(variance + 1e-05)
        pred = jnp.dot(inputs_here, proj_weight, preferred_element_type=jnp.float32) + proj_bias
        differ = pred - tnorm
        magnitude = jnp.abs(differ)
        smooth = jnp.where(magnitude < 1.0, 0.5 * differ * differ, magnitude - 0.5)
        clipped = coverage * jnp.clip(differ, -1.0, 1.0)
        source = clipped.astype(jnp.bfloat16)
        grad_acc = grad_acc + lax.dot_general(inputs_here, source, (((0,), (0,)), ((), ())), preferred_element_type=jnp.float32)
        bias_acc = bias_acc + lax.optimization_barrier(jnp.sum(clipped, axis=0))
        loss_acc = loss_acc + jnp.sum(coverage * smooth)
        count_acc = count_acc + jnp.sum(coverage)
        return ((grad_acc, bias_acc, loss_acc, count_acc), None)
    start = (jnp.zeros((E, D), jnp.float32), jnp.zeros((D,), jnp.float32), jnp.zeros((), jnp.float32), jnp.zeros((), jnp.float32))
    (grad_acc, bias_acc, loss_acc, total), unused = lax.scan(step, start, (inputs_grouped, targets_grouped, coverage_grouped))
    grad_w = grad_acc / total
    grad_b = bias_acc / total
    norm = jnp.sqrt(jnp.sum(grad_w * grad_w) + jnp.sum(grad_b * grad_b))
    clip_scale = jnp.minimum(1.0, 1.0 / (norm + 1e-06))
    loss = loss_acc / total / D
    return (loss, clip_scale, clip_scale * grad_w, clip_scale * grad_b)
```

```python
import jax
import jax.numpy as jnp
from jax import lax
from jax.experimental import pallas as pl
from jax.experimental.pallas import tpu as pltpu
from jax.sharding import PartitionSpec as P

MESH = pl.DeviceIdType.MESH
F32 = jnp.float32
BF16 = jnp.bfloat16

NY, NZ, NC, NX = 4, 4, 2, 4
NCHIP = NY * NZ
NDP = NCHIP * NC
GI = 4
NG = 16
IMG = GI * NG
PAT = 256
FEAT = 320
FULL = FEAT * NX
E = 384
ROWS = E // NDP
FP = 384
RB = 64
EARLY = 6

OFFSETS = sorted(
    [(dy, dz) for dy in range(NY) for dz in range(NZ) if (dy, dz) != (0, 0)],
    key=lambda o: -(min(o[0], NY - o[0]) + min(o[1], NZ - o[1])),
)


def kernel(
    x_hbm, w_hbm, b_hbm, t_hbm, m_hbm,
    loss_o, clip_o, gw_o, gb_o,
    xv, tv, mv, wi, wtmp, wg, wsq, wt, bi, bias, pm,
    st_own, st_in, ab, cb, vb, pscr, sscr, acc, gbt, lacc, gt, sb, pin, ps, rr, na, nb,
    x_sem, t_sem, misc_sem,
    st_send, st_recv, w_send, w_recv, c_send, c_recv, r_send, r_recv, a_send, a_recv, b_send, b_recv,
):
    me = lax.axis_index("dp")
    mx = lax.axis_index("mp")
    core = lax.rem(me, NC)
    chip = lax.div(me, NC)
    my_y = lax.div(chip, NZ)
    my_z = lax.rem(chip, NZ)
    partner = me + 1 - 2 * core

    def chip_at(dy, dz):
        return lax.rem(my_y + dy, NY) * NZ + lax.rem(my_z + dz, NZ)

    w_copy = pltpu.make_async_copy(w_hbm, wi, misc_sem.at[0])
    w_copy.start()

    def t_copy(g):
        return pltpu.make_async_copy(
            t_hbm.at[pl.ds(g * GI, GI)], tv.at[pl.ds(g * GI, GI)], t_sem.at[g]
        )

    def x_copy(g):
        return pltpu.make_async_copy(
            x_hbm.at[pl.ds(g * GI, GI)], xv.at[pl.ds(g * GI, GI)], x_sem.at[g]
        )

    def start_t(g, _):
        t_copy(g).start()
        return 0

    lax.fori_loop(0, NG, start_t, 0)
    m_copy = pltpu.make_async_copy(m_hbm, mv, misc_sem.at[1])
    m_copy.start()
    b_copy = pltpu.make_async_copy(b_hbm, bi, misc_sem.at[2])
    b_copy.start()

    barrier = pltpu.get_barrier_semaphore()
    for dy, dz in OFFSETS:
        for c in range(NC):
            pl.semaphore_signal(
                barrier, inc=1, device_id=(chip_at(dy, dz) * NC + c, mx), device_id_type=MESH
            )
    pl.semaphore_signal(barrier, inc=1, device_id=(partner, mx), device_id_type=MESH)
    for dx in range(1, NX):
        for c in range(NC):
            pl.semaphore_signal(
                barrier, inc=1,
                device_id=(chip * NC + c, lax.rem(mx + dx, NX)), device_id_type=MESH,
            )

    w_copy.wait()
    wtmp[...] = jnp.zeros_like(wtmp)
    wtmp[0:ROWS, :] = wi[...].astype(F32)
    wg[me] = wtmp[...].astype(BF16)
    b_copy.wait()

    row = lax.broadcasted_iota(jnp.int32, (E, NDP * 16), 0)
    col = lax.broadcasted_iota(jnp.int32, (E, NDP * 16), 1)
    low = lax.bitwise_and(col, 15)
    pick = (row == lax.shift_right_logical(col, 4) * ROWS + low) & (low < ROWS)
    pm[...] = jnp.where(pick, 1.0, 0.0).astype(BF16)
    wsq[...] = jnp.zeros_like(wsq)
    wsq[0:8, 0:FEAT] = jnp.broadcast_to(bi[...], (8, FEAT))
    bcol = jnp.transpose(jnp.broadcast_to(wsq[0:1, :], (128, FP)))
    bias[...] = bcol[0:FEAT, :]
    acc[...] = jnp.zeros_like(acc)
    gbt[...] = jnp.zeros_like(gbt)
    lacc[...] = jnp.zeros_like(lacc)
    sscr[...] = jnp.zeros_like(sscr)

    def stats(g):
        t_copy(g).wait()
        x_copy(g).start()
        sums, squares = [], []
        for k in range(GI):
            s8 = jnp.zeros((8, PAT), F32)
            q8 = jnp.zeros((8, PAT), F32)
            for r in range(0, FEAT, RB):
                t = tv[g * GI + k, r : r + RB, :].astype(F32).reshape(RB // 8, 8, PAT)
                s8 = s8 + jnp.sum(t, axis=0)
                q8 = q8 + jnp.sum(t * t, axis=0)
            sums.append(jnp.sum(s8, axis=0, keepdims=True))
            squares.append(jnp.sum(q8, axis=0, keepdims=True))
        st_own[g] = jnp.concatenate(sums + squares, axis=0)

    def st_copy(g, p):
        return pltpu.make_async_remote_copy(
            src_ref=st_own.at[g],
            dst_ref=st_in.at[p - 1, g],
            send_sem=st_send.at[p - 1, g],
            recv_sem=st_recv.at[p - 1, g],
            device_id=(me, lax.rem(mx + p, NX)),
            device_id_type=MESH,
        )

    def send_stats(g):
        for p in (2, 1, 3):
            st_copy(g, p).start()

    def stats_only(g, _):
        stats(g)
        return 0

    lax.fori_loop(0, EARLY, stats_only, 0)
    pl.semaphore_wait(barrier, (NCHIP - 1) * NC + 1 + (NX - 1) * NC)

    def w_dst(n):
        return pltpu.make_async_remote_copy(
            src_ref=wg.at[me],
            dst_ref=wg.at[me],
            send_sem=w_send,
            recv_sem=w_recv,
            device_id=(n, mx),
            device_id_type=MESH,
        )

    for dy, dz in OFFSETS:
        for c in range(NC):
            w_dst(chip_at(dy, dz) * NC + c).start()
    w_dst(partner).start()

    def send_early(g, _):
        send_stats(g)
        return 0

    lax.fori_loop(0, EARLY - 1, send_early, 0)

    def stats_and_send(g, _):
        stats(g)
        send_stats(g - 1)
        return 0

    lax.fori_loop(EARLY, NG, stats_and_send, 0)

    m_copy.wait()

    def cover(i, total):
        v = jnp.sum(mv[i].astype(F32), axis=0, keepdims=True)
        vb[i] = jnp.broadcast_to(v, (8, PAT))
        return total + v

    counts = lax.fori_loop(0, IMG, cover, jnp.zeros((1, PAT), F32))
    send_stats(NG - 1)

    def prepare(g):
        for p in (1, 2, 3):
            st_copy(g, p).wait_recv()
        st = (st_own[g] + st_in[0, g]) + (st_in[1, g] + st_in[2, g])
        mean = st[0:GI] * (1.0 / FULL)
        var = jnp.maximum(st[GI : 2 * GI] * (1.0 / FULL) - mean * mean, 0.0)
        a = lax.rsqrt(var + 1e-05)
        c = mean * a
        for k in range(GI):
            ab[g * GI + k] = jnp.broadcast_to(a[k : k + 1], (8, PAT))
            cb[g * GI + k] = jnp.broadcast_to(c[k : k + 1], (8, PAT))

    whole = wg.at[pl.ds(0, NDP - 1)]
    pltpu.make_async_copy(whole, whole, w_recv).wait()
    pltpu.make_async_copy(whole, whole, w_send).wait()

    wsq[:, 0:FEAT] = jnp.dot(
        pm[...], wg[...].reshape(NDP * 16, FEAT), preferred_element_type=F32
    )
    wt[...] = jnp.transpose(wsq[...])[0:FEAT, :].astype(BF16)

    def first(g):
        for k in range(GI):
            pscr[:, k * PAT : (k + 1) * PAT] = lax.dot_general(
                wt[...], xv[g * GI + k], (((1,), (1,)), ((), ())), preferred_element_type=F32
            )

    def second(g):
        xs = xv[pl.ds(g * GI, GI)].reshape(GI * PAT, E)
        acc[0:FEAT, 0:E] += jnp.dot(sscr[...], xs, preferred_element_type=F32)

    def middle(g):
        loss8 = jnp.zeros((8, PAT), F32)
        for r in range(0, FEAT, RB):
            bb = bias[r : r + RB, :]
            b2 = jnp.concatenate([bb, bb], axis=1).reshape(RB // 8, 8, PAT)
            gsum = jnp.zeros((RB // 8, 8, PAT), F32)
            for k in range(GI):
                i = g * GI + k
                a = ab[i][None]
                c = cb[i][None]
                v = vb[i][None]
                p = pscr[r : r + RB, k * PAT : (k + 1) * PAT].reshape(RB // 8, 8, PAT)
                t = tv[i, r : r + RB, :].astype(F32).reshape(RB // 8, 8, PAT)
                d = (p + b2) - (t * a - c)
                h = jnp.minimum(jnp.maximum(d, -1.0), 1.0)
                s = v * h
                loss8 = loss8 + jnp.sum(s * (d - 0.5 * h), axis=0)
                gsum = gsum + s
                sscr[r : r + RB, k * PAT : (k + 1) * PAT] = s.reshape(RB, PAT).astype(BF16)
            gs = gsum.reshape(RB, PAT)
            acc[r : r + RB, E : E + 128] += gs[:, 0:128] + gs[:, 128:256]
        lacc[...] += loss8

    x_copy(0).wait()
    first(0)
    prepare(0)

    def main(g, _):
        nxt = jnp.minimum(g + 1, NG - 1)

        @pl.when(g < NG - 1)
        def _():
            x_copy(nxt).wait()
            prepare(nxt)

        second(jnp.maximum(g - 1, 0))
        middle(g)
        first(nxt)
        return 0

    lax.fori_loop(0, NG, main, 0)
    second(NG - 1)

    gt[...] = jnp.transpose(acc[...])
    gb = jnp.sum(gt[E : E + 128, :], axis=0, keepdims=True)
    loss_all = jnp.sum(lacc[...])
    count_all = jnp.sum(counts)
    lane = lax.broadcasted_iota(jnp.int32, (1, 128), 1)
    tail = jnp.where(lane < 64, gb[:, 256:384], jnp.where(lane < 96, loss_all, count_all))
    for j in range(NDP):
        r = j * ROWS
        slot = sb.at[j % NC, j // NC]
        slot[0:ROWS, :] = gt[r : r + ROWS, 0:128]
        slot[ROWS : 2 * ROWS, :] = gt[r : r + ROWS, 128:256]
        half = ROWS // 2
        up = gt[r : r + half, 256:384]
        down = gt[r + half : r + ROWS, 256:384]
        slot[2 * ROWS : 2 * ROWS + half, :] = up + pltpu.roll(down, 64, 1)
        slot[30:31, :] = gb[:, 0:128]
        slot[31:32, :] = gb[:, 128:256]
        slot[32:40, :] = jnp.broadcast_to(tail, (8, 128))

    pair = pltpu.make_async_remote_copy(
        src_ref=sb.at[1 - core], dst_ref=pin, send_sem=c_send, recv_sem=c_recv,
        device_id=(partner, mx), device_id_type=MESH,
    )
    pair.start()
    pair.wait()
    ps[...] = sb[core] + pin[...]
    rr[chip] = ps[chip]

    def r_copy(n):
        return pltpu.make_async_remote_copy(
            src_ref=ps.at[n], dst_ref=rr.at[chip], send_sem=r_send, recv_sem=r_recv,
            device_id=(n * NC + core, mx), device_id_type=MESH,
        )

    for dy, dz in OFFSETS:
        r_copy(chip_at(dy, dz)).start()
    others = rr.at[pl.ds(0, NCHIP - 1)]
    pltpu.make_async_copy(others, others, r_recv).wait()
    mine = jnp.sum(rr[...], axis=0)
    gbl = mine[30:33]
    lane3 = lax.broadcasted_iota(jnp.int32, (3, 128), 1)
    row3 = lax.broadcasted_iota(jnp.int32, (3, 128), 0)
    gbz = jnp.where((row3 < 2) | (lane3 < 64), gbl, 0.0)
    square = jnp.sum(mine[0:30] * mine[0:30]) + jnp.sum(gbz * gbz) * (1.0 / NDP)
    lrow = mine[32:33, :]
    loss_plane = jnp.sum(jnp.where(lane == 64, lrow, 0.0))
    count = jnp.sum(jnp.where(lane == 96, lrow, 0.0))
    lane8 = lax.broadcasted_iota(jnp.int32, (8, 128), 1)
    mine_a = mx * NC + core
    na[mine_a] = jnp.where(lane8 < 64, square, loss_plane)

    def a_copy(dx, c):
        return pltpu.make_async_remote_copy(
            src_ref=na.at[mine_a], dst_ref=na.at[mine_a], send_sem=a_send, recv_sem=a_recv,
            device_id=(chip * NC + c, lax.rem(mx + dx, NX)), device_id_type=MESH,
        )

    for dx in (2, 1, 3):
        for c in range(NC):
            a_copy(dx, c).start()
    a_copy(0, 1 - core).start()
    rest = na.at[pl.ds(0, NX * NC - 1)]
    pltpu.make_async_copy(rest, rest, a_recv).wait()
    line = jnp.sum(na[...], axis=0)
    loss_sum = jnp.sum(jnp.where(lane == 64, line[0:1], 0.0)) * 0.5
    nb[chip] = line

    def b_out(n):
        return pltpu.make_async_remote_copy(
            src_ref=nb.at[chip], dst_ref=nb.at[chip], send_sem=b_send, recv_sem=b_recv,
            device_id=(n * NC + core, mx), device_id_type=MESH,
        )

    for dy, dz in OFFSETS:
        b_out(chip_at(dy, dz)).start()
    rest_b = nb.at[pl.ds(0, NCHIP - 1)]
    pltpu.make_async_copy(rest_b, rest_b, b_recv).wait()
    final = jnp.sum(nb[...], axis=0)
    total = jnp.broadcast_to(final[0:1, 0:1], (1, 128))
    countv = jnp.full((1, 128), count, F32)
    norm = jnp.sqrt(total) / countv
    clip = jnp.minimum(1.0, 1.0 / (norm + 1e-06))
    factor = clip / countv
    clip_o[...] = clip[:, 0:1]
    loss_o[...] = (jnp.full((1, 128), loss_sum, F32) / countv * (1.0 / FULL))[:, 0:1]
    out = mine * factor
    gw_o[:, 0:128] = out[0:ROWS]
    gw_o[:, 128:256] = out[ROWS : 2 * ROWS]
    half = ROWS // 2
    gw_o[0:half, 256:320] = out[2 * ROWS : 2 * ROWS + half, 0:64]
    gw_o[half:ROWS, 256:320] = out[2 * ROWS : 2 * ROWS + half, 64:128]
    gb_o[:, 0:128] = out[30:31]
    gb_o[:, 128:256] = out[31:32]
    gb_o[:, 256:320] = out[32:33, 0:64]

    def drain(g, _):
        for p in (1, 2, 3):
            st_copy(g, p).wait_send()
        return 0

    lax.fori_loop(0, NG, drain, 0)
    sent = ps.at[pl.ds(0, NCHIP - 1)]
    pltpu.make_async_copy(sent, sent, r_send).wait()
    pltpu.make_async_copy(rest, rest, a_send).wait()
    pltpu.make_async_copy(rest_b, rest_b, b_send).wait()


def body(pred_input, proj_weight, proj_bias, targets, block_masks):
    any_spec = pl.BlockSpec(memory_space=pl.ANY)
    vmem_spec = pl.BlockSpec(memory_space=pltpu.VMEM)
    vm = pltpu.VMEM
    dma = pltpu.SemaphoreType.DMA
    loss, clip, gw, gb = pl.pallas_call(
        kernel,
        name="fused",
        out_shape=(
            jax.ShapeDtypeStruct((1, 1), F32),
            jax.ShapeDtypeStruct((1, 1), F32),
            jax.ShapeDtypeStruct((ROWS, FEAT), F32),
            jax.ShapeDtypeStruct((1, FEAT), F32),
        ),
        in_specs=[any_spec] * 5,
        out_specs=(vmem_spec,) * 4,
        scratch_shapes=[
            vm((IMG, PAT, E), BF16),
            vm((IMG, FEAT, PAT), BF16),
            vm((IMG, 4, PAT), jnp.int32),
            vm((ROWS, FEAT), BF16),
            vm((16, FEAT), F32),
            vm((NDP, 16, FEAT), BF16),
            vm((E, FP), F32),
            vm((FEAT, E), BF16),
            vm((1, FEAT), F32),
            vm((FEAT, 128), F32),
            vm((E, NDP * 16), BF16),
            vm((NG, 2 * GI, PAT), F32),
            vm((NX - 1, NG, 2 * GI, PAT), F32),
            vm((IMG, 8, PAT), F32),
            vm((IMG, 8, PAT), F32),
            vm((IMG, 8, PAT), F32),
            vm((FEAT, GI * PAT), F32),
            vm((FEAT, GI * PAT), BF16),
            vm((FP, E + 128), F32),
            vm((8, 128), F32),
            vm((8, PAT), F32),
            vm((E + 128, FP), F32),
            vm((NC, NCHIP, 40, 128), F32),
            vm((NCHIP, 40, 128), F32),
            vm((NCHIP, 40, 128), F32),
            vm((NCHIP, 40, 128), F32),
            vm((NX * NC, 8, 128), F32),
            vm((NCHIP, 8, 128), F32),
            dma((NG,)), dma((NG,)), dma((3,)),
            dma((NX - 1, NG)), dma((NX - 1, NG)),
            dma, dma, dma, dma, dma, dma, dma, dma, dma, dma,
        ],
        compiler_params=pltpu.CompilerParams(
            collective_id=0, has_side_effects=True, vmem_limit_bytes=64 * 1024 * 1024 - 65536,
        ),
    )(
        pred_input,
        proj_weight,
        proj_bias.reshape(1, FEAT),
        jnp.swapaxes(targets, 1, 2),
        block_masks,
    )
    return loss.reshape(()), clip.reshape(()), gw, gb.reshape(FEAT)


def solution(mesh):
    return jax.shard_map(
        body,
        mesh=mesh,
        in_specs=(
            P("dp", None, None), P("dp", "mp"), P("mp"), P("dp", None, "mp"), P("dp", None, None),
        ),
        out_specs=(P(), P(), P("dp", "mp"), P("mp")),
        check_vma=False,
    )
```

```python
import jax
import jax.numpy as jnp
from jax import lax
from jax.experimental import pallas as pl
from jax.experimental.pallas import tpu as pltpu
from jax.sharding import PartitionSpec as P

MESH = pl.DeviceIdType.MESH
F32 = jnp.float32
BF16 = jnp.bfloat16

NY, NZ, NC, NX = 4, 4, 2, 4
NCHIP = NY * NZ
NDP = NCHIP * NC
GI = 4
NG = 16
IMG = GI * NG
PAT = 256
FEAT = 320
FULL = FEAT * NX
E = 384
ROWS = E // NDP
FP = 384
RB = 64
EARLY = 6

EVERY = sorted(
    [
        (dx, dy, dz)
        for dx in range(NX) for dy in range(NY) for dz in range(NZ)
        if (dx, dy, dz) != (0, 0, 0)
    ],
    key=lambda o: -(min(o[0], NX - o[0]) + min(o[1], NY - o[1]) + min(o[2], NZ - o[2])),
)
OFFSETS = sorted(
    [(dy, dz) for dy in range(NY) for dz in range(NZ) if (dy, dz) != (0, 0)],
    key=lambda o: -(min(o[0], NY - o[0]) + min(o[1], NZ - o[1])),
)


def kernel(
    x_hbm, w_hbm, b_hbm, t_hbm, m_hbm,
    out_o,
    xv, tv, mv, wi, wtmp, wg, wsq, wt, bi, bias, wide,
    st_own, st_in, ab, cb, vb, pscr, sscr, acc, lacc, gt, sb, pin, ps, rr, nb,
    x_sem, t_sem, misc_sem,
    st_send, st_recv, w_send, w_recv, c_send, c_recv, r_send, r_recv, b_send, b_recv,
):
    me = lax.axis_index("dp")
    mx = lax.axis_index("mp")
    core = lax.rem(me, NC)
    chip = lax.div(me, NC)
    my_y = lax.div(chip, NZ)
    my_z = lax.rem(chip, NZ)
    partner = me + 1 - 2 * core

    def chip_at(dy, dz):
        return lax.rem(my_y + dy, NY) * NZ + lax.rem(my_z + dz, NZ)

    barrier = pltpu.get_barrier_semaphore()
    for dy, dz in OFFSETS:
        for c in range(NC):
            pl.semaphore_signal(
                barrier, inc=1, device_id=(chip_at(dy, dz) * NC + c, mx), device_id_type=MESH
            )
    pl.semaphore_signal(barrier, inc=1, device_id=(partner, mx), device_id_type=MESH)
    for dx in range(1, NX):
        pl.semaphore_signal(
            barrier, inc=1, device_id=(me, lax.rem(mx + dx, NX)), device_id_type=MESH
        )

    w_copy = pltpu.make_async_copy(w_hbm, wi, misc_sem.at[0])
    w_copy.start()
    b_copy = pltpu.make_async_copy(b_hbm, bi, misc_sem.at[2])
    b_copy.start()

    def t_copy(g):
        return pltpu.make_async_copy(
            t_hbm.at[pl.ds(g * GI, GI)], tv.at[pl.ds(g * GI, GI)], t_sem.at[g]
        )

    def x_copy(g):
        return pltpu.make_async_copy(
            x_hbm.at[pl.ds(g * GI, GI)], xv.at[pl.ds(g * GI, GI)], x_sem.at[g]
        )

    def start_t(g, _):
        t_copy(g).start()
        return 0

    lax.fori_loop(0, NG, start_t, 0)
    m_copy = pltpu.make_async_copy(m_hbm, mv, misc_sem.at[1])
    m_copy.start()

    w_copy.wait()
    wide[...] = jnp.zeros_like(wide)
    wf = wi[...].astype(F32)
    wide[:, 0:FEAT] = wf
    half = ROWS // 2
    wtmp[2 * ROWS : 32, :] = jnp.zeros((32 - 2 * ROWS, 128), F32)
    wtmp[0:ROWS, :] = wide[:, 0:128]
    wtmp[ROWS : 2 * ROWS, :] = wide[:, 128:256]
    wtmp[2 * ROWS : 2 * ROWS + half, :] = wide[0:half, 256:384] + pltpu.roll(
        wide[half:ROWS, 256:384], 64, 1
    )
    wg[me] = wtmp[...].astype(BF16)
    b_copy.wait()

    wsq[...] = jnp.zeros_like(wsq)
    wsq[0:8, 0:FEAT] = jnp.broadcast_to(bi[...].reshape(1, FEAT), (8, FEAT))
    bcol = jnp.transpose(jnp.broadcast_to(wsq[0:1, :], (128, FP)))
    bias[...] = bcol[0:FEAT, :]
    acc[...] = jnp.zeros_like(acc)
    lacc[...] = jnp.zeros_like(lacc)
    sscr[...] = jnp.zeros_like(sscr)

    def stats(g):
        t_copy(g).wait()
        x_copy(g).start()
        sums, squares = [], []
        for k in range(GI):
            s8 = jnp.zeros((8, PAT), F32)
            q8 = jnp.zeros((8, PAT), F32)
            for r in range(0, FEAT, RB):
                t = tv[g * GI + k, r : r + RB, :].astype(F32).reshape(RB // 8, 8, PAT)
                s8 = s8 + jnp.sum(t, axis=0)
                q8 = q8 + jnp.sum(t * t, axis=0)
            sums.append(jnp.sum(s8, axis=0, keepdims=True))
            squares.append(jnp.sum(q8, axis=0, keepdims=True))
        st_own[g] = jnp.concatenate(sums + squares, axis=0)

    def st_copy(g, p):
        return pltpu.make_async_remote_copy(
            src_ref=st_own.at[g],
            dst_ref=st_in.at[p - 1, g],
            send_sem=st_send.at[p - 1, g],
            recv_sem=st_recv.at[p - 1, g],
            device_id=(me, lax.rem(mx + p, NX)),
            device_id_type=MESH,
        )

    def send_stats(g):
        for p in (2, 1, 3):
            st_copy(g, p).start()

    def stats_only(g, _):
        stats(g)
        return 0

    lax.fori_loop(0, EARLY, stats_only, 0)
    pl.semaphore_wait(barrier, (NCHIP - 1) * NC + NX)

    def w_dst(n):
        return pltpu.make_async_remote_copy(
            src_ref=wg.at[me],
            dst_ref=wg.at[me],
            send_sem=w_send,
            recv_sem=w_recv,
            device_id=(n, mx),
            device_id_type=MESH,
        )

    for dy, dz in OFFSETS:
        for c in range(NC):
            w_dst(chip_at(dy, dz) * NC + c).start()
    w_dst(partner).start()

    def send_early(g, _):
        send_stats(g)
        return 0

    lax.fori_loop(0, EARLY - 1, send_early, 0)

    def stats_and_send(g, _):
        stats(g)
        send_stats(g - 1)
        return 0

    lax.fori_loop(EARLY, NG, stats_and_send, 0)

    m_copy.wait()

    def cover(i, total):
        v = jnp.sum(mv[i].astype(F32), axis=0, keepdims=True)
        vb[i] = jnp.broadcast_to(v, (8, PAT))
        return total + v

    counts = lax.fori_loop(0, IMG, cover, jnp.zeros((1, PAT), F32))
    send_stats(NG - 1)

    def prepare(g):
        for p in (1, 2, 3):
            st_copy(g, p).wait_recv()
        st = (st_own[g] + st_in[0, g]) + (st_in[1, g] + st_in[2, g])
        mean = st[0:GI] * (1.0 / FULL)
        var = jnp.maximum(st[GI : 2 * GI] * (1.0 / FULL) - mean * mean, 0.0)
        a = lax.rsqrt(var + 1e-05)
        c = mean * a
        for k in range(GI):
            ab[g * GI + k] = jnp.broadcast_to(a[k : k + 1], (8, PAT))
            cb[g * GI + k] = jnp.broadcast_to(c[k : k + 1], (8, PAT))

    whole = wg.at[pl.ds(0, NDP - 1)]
    pltpu.make_async_copy(whole, whole, w_recv).wait()
    pltpu.make_async_copy(whole, whole, w_send).wait()

    left = lax.broadcasted_iota(jnp.int32, (half, 128), 1) < 64
    for j in range(NDP):
        r = j * ROWS
        wtmp[...] = wg[j].astype(F32)
        wsq[r : r + ROWS, 0:128] = wtmp[0:ROWS, :]
        wsq[r : r + ROWS, 128:256] = wtmp[ROWS : 2 * ROWS, :]
        both = wtmp[2 * ROWS : 2 * ROWS + half, :]
        wsq[r : r + half, 256:384] = jnp.where(left, both, 0.0)
        wsq[r + half : r + ROWS, 256:384] = jnp.where(left, pltpu.roll(both, 64, 1), 0.0)
    wt[...] = jnp.transpose(wsq[...])[0:FEAT, :].astype(BF16)

    def first(g):
        for k in range(GI):
            pscr[:, k * PAT : (k + 1) * PAT] = lax.dot_general(
                wt[...], xv[g * GI + k], (((1,), (1,)), ((), ())), preferred_element_type=F32
            )

    def second(g):
        xs = xv[pl.ds(g * GI, GI)].reshape(GI * PAT, E)
        acc[0:FEAT, 0:E] += jnp.dot(sscr[...], xs, preferred_element_type=F32)

    def middle(g):
        loss8 = jnp.zeros((8, PAT), F32)
        for r in range(0, FEAT, RB):
            bb = bias[r : r + RB, :]
            b2 = jnp.concatenate([bb, bb], axis=1).reshape(RB // 8, 8, PAT)
            gsum = jnp.zeros((RB // 8, 8, PAT), F32)
            for k in range(GI):
                i = g * GI + k
                a = ab[i][None]
                c = cb[i][None]
                v = vb[i][None]
                p = pscr[r : r + RB, k * PAT : (k + 1) * PAT].reshape(RB // 8, 8, PAT)
                t = tv[i, r : r + RB, :].astype(F32).reshape(RB // 8, 8, PAT)
                d = (p + b2) - (t * a - c)
                h = jnp.minimum(jnp.maximum(d, -1.0), 1.0)
                s = v * h
                loss8 = loss8 + jnp.sum(s * (d - 0.5 * h), axis=0)
                gsum = gsum + s
                sscr[r : r + RB, k * PAT : (k + 1) * PAT] = s.reshape(RB, PAT).astype(BF16)
            gs = gsum.reshape(RB, PAT)
            acc[r : r + RB, E : E + 128] += gs[:, 0:128] + gs[:, 128:256]
        lacc[...] += loss8

    x_copy(0).wait()
    first(0)
    prepare(0)

    def main(g, _):
        nxt = jnp.minimum(g + 1, NG - 1)

        @pl.when(g < NG - 1)
        def _():
            x_copy(nxt).wait()
            prepare(nxt)

        second(jnp.maximum(g - 1, 0))
        middle(g)
        first(nxt)
        return 0

    lax.fori_loop(0, NG, main, 0)
    second(NG - 1)

    gt[...] = jnp.transpose(acc[...])
    gb = jnp.sum(gt[E : E + 128, :], axis=0, keepdims=True)
    loss_all = jnp.sum(lacc[...])
    count_all = jnp.sum(counts)
    lane = lax.broadcasted_iota(jnp.int32, (1, 128), 1)
    tail = jnp.where(lane < 64, gb[:, 256:384], jnp.where(lane < 96, loss_all, count_all))
    for j in range(NDP):
        r = j * ROWS
        slot = sb.at[j % NC, j // NC]
        slot[0:ROWS, :] = gt[r : r + ROWS, 0:128]
        slot[ROWS : 2 * ROWS, :] = gt[r : r + ROWS, 128:256]
        half = ROWS // 2
        up = gt[r : r + half, 256:384]
        down = gt[r + half : r + ROWS, 256:384]
        slot[2 * ROWS : 2 * ROWS + half, :] = up + pltpu.roll(down, 64, 1)
        slot[30:31, :] = gb[:, 0:128]
        slot[31:32, :] = gb[:, 128:256]
        slot[32:40, :] = jnp.broadcast_to(tail, (8, 128))

    pair = pltpu.make_async_remote_copy(
        src_ref=sb.at[1 - core], dst_ref=pin, send_sem=c_send, recv_sem=c_recv,
        device_id=(partner, mx), device_id_type=MESH,
    )
    pair.start()
    pair.wait()
    ps[...] = sb[core] + pin[...]
    rr[chip] = ps[chip]

    def r_copy(n):
        return pltpu.make_async_remote_copy(
            src_ref=ps.at[n], dst_ref=rr.at[chip], send_sem=r_send, recv_sem=r_recv,
            device_id=(n * NC + core, mx), device_id_type=MESH,
        )

    for dy, dz in OFFSETS:
        r_copy(chip_at(dy, dz)).start()
    others = rr.at[pl.ds(0, NCHIP - 1)]
    pltpu.make_async_copy(others, others, r_recv).wait()
    mine = jnp.sum(rr[...], axis=0)
    gbl = mine[30:33]
    lane3 = lax.broadcasted_iota(jnp.int32, (3, 128), 1)
    row3 = lax.broadcasted_iota(jnp.int32, (3, 128), 0)
    gbz = jnp.where((row3 < 2) | (lane3 < 64), gbl, 0.0)
    square = jnp.sum(mine[0:30] * mine[0:30]) + jnp.sum(gbz * gbz) * (1.0 / NDP)
    lrow = mine[32:33, :]
    loss_plane = jnp.sum(jnp.where(lane == 64, lrow, 0.0))
    count = jnp.sum(jnp.where(lane == 96, lrow, 0.0))
    ident = me * NX + mx
    nb[ident] = jnp.where(lane < 64, square, loss_plane)

    def b_out(n, m):
        return pltpu.make_async_remote_copy(
            src_ref=nb.at[ident], dst_ref=nb.at[ident], send_sem=b_send, recv_sem=b_recv,
            device_id=(n, m), device_id_type=MESH,
        )

    for dx, dy, dz in EVERY:
        for c in range(NC):
            b_out(chip_at(dy, dz) * NC + c, lax.rem(mx + dx, NX)).start()
    b_out(partner, mx).start()
    rest_b = nb.at[pl.ds(0, NDP * NX - 1)]
    pltpu.make_async_copy(rest_b, rest_b, b_recv).wait()
    parts = [jnp.sum(nb[16 * q : 16 * q + 16], axis=0) for q in range(NDP * NX // 16)]
    final = ((parts[0] + parts[1]) + (parts[2] + parts[3])) + (
        (parts[4] + parts[5]) + (parts[6] + parts[7])
    )
    loss_sum = jnp.sum(jnp.where(lane == 64, final, 0.0)) * (1.0 / NDP)
    total = jnp.broadcast_to(final[0:1, 0:1], (1, 128))
    countv = jnp.full((1, 128), count, F32)
    norm = jnp.sqrt(total) / countv
    clip = jnp.minimum(1.0, 1.0 / (norm + 1e-06))
    factor = clip / countv
    row40 = lax.broadcasted_iota(jnp.int32, (40, 128), 0)
    loss = jnp.full((1, 128), loss_sum, F32) / countv * (1.0 / FULL)
    out_o[...] = jnp.where(row40 == 33, loss, jnp.where(row40 == 34, clip, mine * factor))

    def drain(g, _):
        for p in (1, 2, 3):
            st_copy(g, p).wait_send()
        return 0

    lax.fori_loop(0, NG, drain, 0)
    sent = ps.at[pl.ds(0, NCHIP - 1)]
    pltpu.make_async_copy(sent, sent, r_send).wait()
    pltpu.make_async_copy(rest_b, rest_b, b_send).wait()


def spread(in_ref, loss_o, clip_o, gw_o, gb_o):
    half = ROWS // 2
    gw_o[:, 0:128] = in_ref[0:ROWS]
    gw_o[:, 128:256] = in_ref[ROWS : 2 * ROWS]
    gw_o[0:half, 256:320] = in_ref[2 * ROWS : 2 * ROWS + half, 0:64]
    gw_o[half:ROWS, 256:320] = in_ref[2 * ROWS : 2 * ROWS + half, 64:128]
    gb_o[...] = jnp.concatenate(
        [in_ref[30:31, :], in_ref[31:32, :], in_ref[32:33, 0:64]], axis=1
    ).reshape(FEAT)
    loss_o[...] = in_ref[33:34, 0:1]
    clip_o[...] = in_ref[34:35, 0:1]


def body(pred_input, proj_weight, proj_bias, targets, block_masks):
    any_spec = pl.BlockSpec(memory_space=pl.ANY)
    vmem_spec = pl.BlockSpec(memory_space=pltpu.VMEM)
    vm = pltpu.VMEM
    dma = pltpu.SemaphoreType.DMA
    packed = pl.pallas_call(
        kernel,
        name="fused",
        out_shape=jax.ShapeDtypeStruct((40, 128), F32),
        in_specs=[any_spec] * 5,
        out_specs=vmem_spec,
        scratch_shapes=[
            vm((IMG, PAT, E), BF16),
            vm((IMG, FEAT, PAT), BF16),
            vm((IMG, 4, PAT), jnp.int32),
            vm((ROWS, FEAT), BF16),
            vm((32, 128), F32),
            vm((NDP, 32, 128), BF16),
            vm((E, FP), F32),
            vm((FEAT, E), BF16),
            vm((FEAT,), F32),
            vm((FEAT, 128), F32),
            vm((ROWS, FP), F32),
            vm((NG, 2 * GI, PAT), F32),
            vm((NX - 1, NG, 2 * GI, PAT), F32),
            vm((IMG, 8, PAT), F32),
            vm((IMG, 8, PAT), F32),
            vm((IMG, 8, PAT), F32),
            vm((FEAT, GI * PAT), F32),
            vm((FEAT, GI * PAT), BF16),
            vm((FP, E + 128), F32),
            vm((8, PAT), F32),
            vm((E + 128, FP), F32),
            vm((NC, NCHIP, 40, 128), F32),
            vm((NCHIP, 40, 128), F32),
            vm((NCHIP, 40, 128), F32),
            vm((NCHIP, 40, 128), F32),
            vm((NDP * NX, 1, 128), F32),
            dma((NG,)), dma((NG,)), dma((3,)),
            dma((NX - 1, NG)), dma((NX - 1, NG)),
            dma, dma, dma, dma, dma, dma, dma, dma,
        ],
        compiler_params=pltpu.CompilerParams(
            collective_id=0, has_side_effects=True, vmem_limit_bytes=64 * 1024 * 1024 - 65536,
        ),
    )(
        pred_input,
        proj_weight,
        proj_bias,
        jnp.swapaxes(targets, 1, 2),
        block_masks,
    )
    loss, clip, gw, gb = pl.pallas_call(
        spread,
        name="spread",
        out_shape=(
            jax.ShapeDtypeStruct((1, 1), F32),
            jax.ShapeDtypeStruct((1, 1), F32),
            jax.ShapeDtypeStruct((ROWS, FEAT), F32),
            jax.ShapeDtypeStruct((FEAT,), F32),
        ),
        in_specs=[vmem_spec],
        out_specs=(vmem_spec,) * 4,
    )(packed)
    return loss.reshape(()), clip.reshape(()), gw, gb


def solution(mesh):
    return jax.shard_map(
        body,
        mesh=mesh,
        in_specs=(
            P("dp", None, None), P("dp", "mp"), P("mp"), P("dp", None, "mp"), P("dp", None, None),
        ),
        out_specs=(P(), P(), P("dp", "mp"), P("mp")),
        check_vma=False,
    )
```

```python
import jax
import jax.numpy as jnp
from jax import lax
from jax.experimental import pallas as pl
from jax.experimental.pallas import tpu as pltpu
from jax.sharding import PartitionSpec as P

MESH = pl.DeviceIdType.MESH
F32 = jnp.float32
BF16 = jnp.bfloat16

NY, NZ, NC, NX = 4, 4, 2, 4
NCHIP = NY * NZ
NDP = NCHIP * NC
GI = 4
NG = 16
IMG = GI * NG
PAT = 256
FEAT = 320
FULL = FEAT * NX
E = 384
ROWS = E // NDP
FP = 384
RB = 64
XW = 512

EVERY = sorted(
    [
        (dx, dy, dz)
        for dx in range(NX) for dy in range(NY) for dz in range(NZ)
        if (dx, dy, dz) != (0, 0, 0)
    ],
    key=lambda o: -(min(o[0], NX - o[0]) + min(o[1], NY - o[1]) + min(o[2], NZ - o[2])),
)
OFFSETS = sorted(
    [(dy, dz) for dy in range(NY) for dz in range(NZ) if (dy, dz) != (0, 0)],
    key=lambda o: -(min(o[0], NY - o[0]) + min(o[1], NZ - o[1])),
)


def kernel(*args):
    pl.run_scoped(
        lambda *refs: work(refs[:-2], refs[-2:], *args),
        *([pltpu.ACC(0)((RB, 256), F32)] * (2 * FEAT // RB) + [pltpu.ACC(1)((FEAT, 256), F32)] * 2),
    )


def work(
    pieces, grad,
    x_hbm, w_hbm, b_hbm, t_hbm, m_hbm,
    out_o,
    xv, tv, mv, wi, wtmp, wg, wsq, wt, bi, wide,
    st_own, st_in, ab, cb, vb, sa, sc, acc, lacc, gt, sb, pin, ps, rr, nb,
    x_sem, t_sem, misc_sem,
    st_send, st_recv, w_send, w_recv, c_send, c_recv, r_send, r_recv, b_send, b_recv,
):
    sets = (pieces[: FEAT // RB], pieces[FEAT // RB :])
    outs = (sa, sc)
    me = lax.axis_index("dp")
    mx = lax.axis_index("mp")
    core = lax.rem(me, NC)
    chip = lax.div(me, NC)
    my_y = lax.div(chip, NZ)
    my_z = lax.rem(chip, NZ)
    partner = me + 1 - 2 * core

    def chip_at(dy, dz):
        return lax.rem(my_y + dy, NY) * NZ + lax.rem(my_z + dz, NZ)

    w_copy = pltpu.make_async_copy(w_hbm, wi, misc_sem.at[0])
    w_copy.start()
    b_copy = pltpu.make_async_copy(b_hbm, bi, misc_sem.at[2])
    b_copy.start()

    barrier = pltpu.get_barrier_semaphore()
    for dy, dz in OFFSETS:
        for c in range(NC):
            pl.semaphore_signal(
                barrier, inc=1, device_id=(chip_at(dy, dz) * NC + c, mx), device_id_type=MESH
            )
    pl.semaphore_signal(barrier, inc=1, device_id=(partner, mx), device_id_type=MESH)
    for dx in range(1, NX):
        pl.semaphore_signal(
            barrier, inc=1, device_id=(me, lax.rem(mx + dx, NX)), device_id_type=MESH
        )

    def t_copy(g):
        return pltpu.make_async_copy(
            t_hbm.at[pl.ds(g * GI, GI)], tv.at[pl.ds(g * GI, GI)], t_sem.at[g]
        )

    def x_copy(g):
        return pltpu.make_async_copy(
            x_hbm.at[pl.ds(g * GI, GI)], xv.at[pl.ds(g * GI, GI), :, pl.ds(0, E)], x_sem.at[g]
        )

    def start_t(g, _):
        t_copy(g).start()
        return 0

    lax.fori_loop(0, NG, start_t, 0)
    m_copy = pltpu.make_async_copy(m_hbm, mv, misc_sem.at[1])
    m_copy.start()

    w_copy.wait()
    wide[...] = jnp.zeros_like(wide)
    wf = wi[...].astype(F32)
    wide[:, 0:FEAT] = wf
    half = ROWS // 2
    wtmp[2 * ROWS : 32, :] = jnp.zeros((32 - 2 * ROWS, 128), F32)
    wtmp[0:ROWS, :] = wide[:, 0:128]
    wtmp[ROWS : 2 * ROWS, :] = wide[:, 128:256]
    wtmp[2 * ROWS : 2 * ROWS + half, :] = wide[0:half, 256:384] + pltpu.roll(
        wide[half:ROWS, 256:384], 64, 1
    )
    wg[me] = wtmp[...].astype(BF16)

    pl.semaphore_wait(barrier, (NCHIP - 1) * NC + NX)

    def w_dst(n):
        return pltpu.make_async_remote_copy(
            src_ref=wg.at[me],
            dst_ref=wg.at[me],
            send_sem=w_send,
            recv_sem=w_recv,
            device_id=(n, mx),
            device_id_type=MESH,
        )

    for dy, dz in OFFSETS:
        for c in range(NC):
            w_dst(chip_at(dy, dz) * NC + c).start()
    w_dst(partner).start()

    b_copy.wait()
    wsq[...] = jnp.zeros_like(wsq)
    b_all = bi[...].reshape(1, FEAT)
    b_high = b_all.astype(BF16).astype(F32)
    b_mid = (b_all - b_high).astype(BF16).astype(F32)
    wsq[E : E + 1, 0:FEAT] = b_high
    wsq[E + 1 : E + 2, 0:FEAT] = b_mid
    wsq[E + 2 : E + 3, 0:FEAT] = (b_all - b_high) - b_mid
    acc[...] = jnp.zeros_like(acc)
    lacc[...] = jnp.zeros_like(lacc)
    sc[...] = jnp.zeros_like(sc)
    none = jnp.zeros((RB, 256), BF16)
    for q in range(2):
        pltpu.matmul_acc_lhs(pieces[0], none, load_staged_rhs=q)
        pltpu.matmul_acc_lhs(grad[0], jnp.zeros((FEAT, 256), BF16), load_staged_rhs=q)
    for piece in (*pieces, *grad):
        pltpu.matmul_pop(piece)


    lane_x = lax.broadcasted_iota(jnp.int32, (1, 1, XW - E), 2)
    ones = jnp.where(lane_x < 3, 1.0, 0.0).astype(BF16)

    def stats(g):
        t_copy(g).wait()
        x_copy(g).start()
        xv[pl.ds(g * GI, GI), :, E:XW] = jnp.broadcast_to(ones, (GI, PAT, XW - E))
        sums, squares = [], []
        for k in range(GI):
            s8 = jnp.zeros((8, PAT), F32)
            q8 = jnp.zeros((8, PAT), F32)
            for r in range(0, FEAT, RB):
                t = tv[g * GI + k, r : r + RB, :].astype(F32).reshape(RB // 8, 8, PAT)
                s8 = s8 + jnp.sum(t, axis=0)
                q8 = q8 + jnp.sum(t * t, axis=0)
            sums.append(jnp.sum(s8, axis=0, keepdims=True))
            squares.append(jnp.sum(q8, axis=0, keepdims=True))
        st_own[g] = jnp.concatenate(sums + squares, axis=0)

    def st_copy(g, p):
        return pltpu.make_async_remote_copy(
            src_ref=st_own.at[g],
            dst_ref=st_in.at[p - 1, g],
            send_sem=st_send.at[p - 1, g],
            recv_sem=st_recv.at[p - 1, g],
            device_id=(me, lax.rem(mx + p, NX)),
            device_id_type=MESH,
        )

    def send_stats(g):
        for p in (2, 1, 3):
            st_copy(g, p).start()

    stats(0)

    def stats_and_send(g, _):
        stats(g)
        send_stats(g - 1)
        return 0

    lax.fori_loop(1, NG, stats_and_send, 0)

    m_copy.wait()

    def cover(i, total):
        v = jnp.sum(mv[i].astype(F32), axis=0, keepdims=True)
        vb[i] = jnp.broadcast_to(v, (8, PAT))
        return total + v

    counts = lax.fori_loop(0, IMG, cover, jnp.zeros((1, PAT), F32))
    send_stats(NG - 1)

    def prepare(g):
        for p in (1, 2, 3):
            st_copy(g, p).wait_recv()
        st = (st_own[g] + st_in[0, g]) + (st_in[1, g] + st_in[2, g])
        mean = st[0:GI] * (1.0 / FULL)
        var = jnp.maximum(st[GI : 2 * GI] * (1.0 / FULL) - mean * mean, 0.0)
        a = lax.rsqrt(var + 1e-05)
        c = mean * a
        for k in range(GI):
            ab[g * GI + k] = jnp.broadcast_to(a[k : k + 1], (8, PAT))
            cb[g * GI + k] = jnp.broadcast_to(c[k : k + 1], (8, PAT))

    whole = wg.at[pl.ds(0, NDP - 1)]
    pltpu.make_async_copy(whole, whole, w_recv).wait()

    left = lax.broadcasted_iota(jnp.int32, (half, 128), 1) < 64
    for j in range(NDP):
        r = j * ROWS
        wtmp[...] = wg[j].astype(F32)
        wsq[r : r + ROWS, 0:128] = wtmp[0:ROWS, :]
        wsq[r : r + ROWS, 128:256] = wtmp[ROWS : 2 * ROWS, :]
        both = wtmp[2 * ROWS : 2 * ROWS + half, :]
        wsq[r : r + half, 256:384] = jnp.where(left, both, 0.0)
        wsq[r + half : r + ROWS, 256:384] = jnp.where(left, pltpu.roll(both, 64, 1), 0.0)
    wt[...] = jnp.transpose(wsq[...])[0:FEAT, :].astype(BF16)

    def first(i, pieces):
        for q in range(2):
            pltpu.matmul_push_rhs(
                xv[i, :, 256 * q : 256 * q + 256], staging_register=q, mxu_index=0, transpose=True
            )
        for q in range(2):
            for n, piece in enumerate(pieces):
                pltpu.matmul_acc_lhs(
                    piece, wt[RB * n : RB * n + RB, 256 * q : 256 * q + 256],
                    load_staged_rhs=q if n == 0 else None,
                )

    def second(i, source):
        for q in range(2):
            pltpu.matmul_push_rhs(
                xv[i, :, 256 * q : 256 * q + 256], staging_register=q, mxu_index=1
            )
        for q in range(2):
            pltpu.matmul_acc_lhs(grad[q], source[...], load_staged_rhs=q)

    def middle(i, pieces, target):
        a = ab[i][None]
        c = cb[i][None]
        v = vb[i][None]
        loss8 = jnp.zeros((8, PAT), F32)
        for n, piece in enumerate(pieces):
            r = RB * n
            p = pltpu.matmul_pop(piece).reshape(RB // 8, 8, PAT)
            t = tv[i, r : r + RB, :].astype(F32).reshape(RB // 8, 8, PAT)
            d = p - (t * a - c)
            h = jnp.minimum(jnp.maximum(d, -1.0), 1.0)
            s = v * h
            loss8 = loss8 + jnp.sum(s * (d - 0.5 * h), axis=0)
            s = s.reshape(RB, PAT)
            target[r : r + RB, :] = s.astype(BF16)
            acc[r : r + RB, E : E + 128] += s[:, 0:128] + s[:, 128:256]
        lacc[...] += loss8

    x_copy(0).wait()
    first(0, sets[0])
    prepare(0)

    def main(g, _):
        nxt = jnp.minimum(g + 1, NG - 1)

        @pl.when(g + 1 < NG)
        def _():
            x_copy(nxt).wait()
            prepare(nxt)

        base = g * GI
        for u in range(GI):
            first(jnp.minimum(base + u + 1, IMG - 1), sets[(u + 1) % 2])
            second(jnp.maximum(base + u - 1, 0), outs[(u + 1) % 2])
            middle(base + u, sets[u % 2], outs[u % 2])
        return 0

    lax.fori_loop(0, NG, main, 0)
    second(IMG - 1, outs[1])
    acc[0:FEAT, 0:256] = pltpu.matmul_pop(grad[0])
    acc[0:FEAT, 256:E] = pltpu.matmul_pop(grad[1])[:, 0:128]
    for piece in sets[0]:
        pltpu.matmul_pop(piece)

    gt[...] = jnp.transpose(acc[...])
    gb = jnp.sum(gt[E : E + 128, :], axis=0, keepdims=True)
    loss_all = jnp.sum(lacc[...])
    count_all = jnp.sum(counts)
    lane = lax.broadcasted_iota(jnp.int32, (1, 128), 1)
    tail = jnp.where(lane < 64, gb[:, 256:384], jnp.where(lane < 96, loss_all, count_all))
    for j in range(NDP):
        r = j * ROWS
        slot = sb.at[j % NC, j // NC]
        slot[0:ROWS, :] = gt[r : r + ROWS, 0:128]
        slot[ROWS : 2 * ROWS, :] = gt[r : r + ROWS, 128:256]
        half = ROWS // 2
        up = gt[r : r + half, 256:384]
        down = gt[r + half : r + ROWS, 256:384]
        slot[2 * ROWS : 2 * ROWS + half, :] = up + pltpu.roll(down, 64, 1)
        slot[30:31, :] = gb[:, 0:128]
        slot[31:32, :] = gb[:, 128:256]
        slot[32:40, :] = jnp.broadcast_to(tail, (8, 128))

    pair = pltpu.make_async_remote_copy(
        src_ref=sb.at[1 - core], dst_ref=pin, send_sem=c_send, recv_sem=c_recv,
        device_id=(partner, mx), device_id_type=MESH,
    )
    pair.start()
    pair.wait()
    ps[...] = sb[core] + pin[...]
    rr[chip] = ps[chip]

    def r_copy(n):
        return pltpu.make_async_remote_copy(
            src_ref=ps.at[n], dst_ref=rr.at[chip], send_sem=r_send, recv_sem=r_recv,
            device_id=(n * NC + core, mx), device_id_type=MESH,
        )

    for dy, dz in OFFSETS:
        r_copy(chip_at(dy, dz)).start()
    others = rr.at[pl.ds(0, NCHIP - 1)]
    pltpu.make_async_copy(others, others, r_recv).wait()
    mine = jnp.sum(rr[...], axis=0)
    gbl = mine[30:33]
    lane3 = lax.broadcasted_iota(jnp.int32, (3, 128), 1)
    row3 = lax.broadcasted_iota(jnp.int32, (3, 128), 0)
    gbz = jnp.where((row3 < 2) | (lane3 < 64), gbl, 0.0)
    square = jnp.sum(mine[0:30] * mine[0:30]) + jnp.sum(gbz * gbz) * (1.0 / NDP)
    lrow = mine[32:33, :]
    loss_plane = jnp.sum(jnp.where(lane == 64, lrow, 0.0))
    count = jnp.sum(jnp.where(lane == 96, lrow, 0.0))
    ident = me * NX + mx
    nb[ident] = jnp.where(lane < 64, square, loss_plane)

    def b_out(n, m):
        return pltpu.make_async_remote_copy(
            src_ref=nb.at[ident], dst_ref=nb.at[ident], send_sem=b_send, recv_sem=b_recv,
            device_id=(n, m), device_id_type=MESH,
        )

    for dx, dy, dz in EVERY:
        for c in range(NC):
            b_out(chip_at(dy, dz) * NC + c, lax.rem(mx + dx, NX)).start()
    b_out(partner, mx).start()
    rest_b = nb.at[pl.ds(0, NDP * NX - 1)]
    pltpu.make_async_copy(rest_b, rest_b, b_recv).wait()
    parts = [jnp.sum(nb[16 * q : 16 * q + 16], axis=0) for q in range(NDP * NX // 16)]
    final = ((parts[0] + parts[1]) + (parts[2] + parts[3])) + (
        (parts[4] + parts[5]) + (parts[6] + parts[7])
    )
    loss_sum = jnp.sum(jnp.where(lane == 64, final, 0.0)) * (1.0 / NDP)
    total = jnp.broadcast_to(final[0:1, 0:1], (1, 128))
    countv = jnp.full((1, 128), count, F32)
    norm = jnp.sqrt(total) / countv
    clip = jnp.minimum(1.0, 1.0 / (norm + 1e-06))
    factor = clip / countv
    row40 = lax.broadcasted_iota(jnp.int32, (40, 128), 0)
    loss = jnp.full((1, 128), loss_sum, F32) / countv * (1.0 / FULL)
    out_o[...] = jnp.where(row40 == 33, loss, jnp.where(row40 == 34, clip, mine * factor))

    def drain(g, _):
        for p in (1, 2, 3):
            st_copy(g, p).wait_send()
        return 0

    lax.fori_loop(0, NG, drain, 0)
    pltpu.make_async_copy(whole, whole, w_send).wait()
    sent = ps.at[pl.ds(0, NCHIP - 1)]
    pltpu.make_async_copy(sent, sent, r_send).wait()
    pltpu.make_async_copy(rest_b, rest_b, b_send).wait()


def spread(in_ref, loss_o, clip_o, gw_o, gb_o):
    half = ROWS // 2
    gw_o[:, 0:128] = in_ref[0:ROWS]
    gw_o[:, 128:256] = in_ref[ROWS : 2 * ROWS]
    gw_o[0:half, 256:320] = in_ref[2 * ROWS : 2 * ROWS + half, 0:64]
    gw_o[half:ROWS, 256:320] = in_ref[2 * ROWS : 2 * ROWS + half, 64:128]
    gb_o[...] = jnp.concatenate(
        [in_ref[30:31, :], in_ref[31:32, :], in_ref[32:33, 0:64]], axis=1
    ).reshape(FEAT)
    loss_o[...] = in_ref[33:34, 0:1]
    clip_o[...] = in_ref[34:35, 0:1]


def body(pred_input, proj_weight, proj_bias, targets, block_masks):
    any_spec = pl.BlockSpec(memory_space=pl.ANY)
    vmem_spec = pl.BlockSpec(memory_space=pltpu.VMEM)
    vm = pltpu.VMEM
    dma = pltpu.SemaphoreType.DMA
    packed = pl.pallas_call(
        kernel,
        name="fused",
        out_shape=jax.ShapeDtypeStruct((40, 128), F32),
        in_specs=[any_spec] * 5,
        out_specs=vmem_spec,
        scratch_shapes=[
            vm((IMG, PAT, XW), BF16),
            vm((IMG, FEAT, PAT), BF16),
            vm((IMG, 4, PAT), jnp.int32),
            vm((ROWS, FEAT), BF16),
            vm((32, 128), F32),
            vm((NDP, 32, 128), BF16),
            vm((XW, FP), F32),
            vm((FEAT, XW), BF16),
            vm((FEAT,), F32),
            vm((ROWS, FP), F32),
            vm((NG, 2 * GI, PAT), F32),
            vm((NX - 1, NG, 2 * GI, PAT), F32),
            vm((IMG, 8, PAT), F32),
            vm((IMG, 8, PAT), F32),
            vm((IMG, 8, PAT), F32),
            vm((FEAT, PAT), BF16),
            vm((FEAT, PAT), BF16),
            vm((FP, E + 128), F32),
            vm((8, PAT), F32),
            vm((E + 128, FP), F32),
            vm((NC, NCHIP, 40, 128), F32),
            vm((NCHIP, 40, 128), F32),
            vm((NCHIP, 40, 128), F32),
            vm((NCHIP, 40, 128), F32),
            vm((NDP * NX, 1, 128), F32),
            dma((NG,)), dma((NG,)), dma((3,)),
            dma((NX - 1, NG)), dma((NX - 1, NG)),
            dma, dma, dma, dma, dma, dma, dma, dma,
        ],
        compiler_params=pltpu.CompilerParams(
            collective_id=0, has_side_effects=True, vmem_limit_bytes=64 * 1024 * 1024 - 65536,
        ),
    )(
        pred_input,
        proj_weight,
        proj_bias,
        jnp.swapaxes(targets, 1, 2),
        block_masks,
    )
    loss, clip, gw, gb = pl.pallas_call(
        spread,
        name="spread",
        out_shape=(
            jax.ShapeDtypeStruct((1, 1), F32),
            jax.ShapeDtypeStruct((1, 1), F32),
            jax.ShapeDtypeStruct((ROWS, FEAT), F32),
            jax.ShapeDtypeStruct((FEAT,), F32),
        ),
        in_specs=[vmem_spec],
        out_specs=(vmem_spec,) * 4,
    )(packed)
    return loss.reshape(()), clip.reshape(()), gw, gb


def solution(mesh):
    return jax.shard_map(
        body,
        mesh=mesh,
        in_specs=(
            P("dp", None, None), P("dp", "mp"), P("mp"), P("dp", None, "mp"), P("dp", None, None),
        ),
        out_specs=(P(), P(), P("dp", "mp"), P("mp")),
        check_vma=False,
    )
```

```python
import jax
import jax.numpy as jnp
from jax import lax
from jax.experimental import pallas as pl
from jax.experimental.pallas import tpu as pltpu
from jax.sharding import PartitionSpec as P

MESH = pl.DeviceIdType.MESH
F32 = jnp.float32
BF16 = jnp.bfloat16

NY, NZ, NC, NX = 4, 4, 2, 4
NCHIP = NY * NZ
NDP = NCHIP * NC
GI = 4
NG = 16
IMG = GI * NG
PAT = 256
FEAT = 320
FULL = FEAT * NX
E = 384
ROWS = E // NDP
FP = 384
RB = 64
XW = 512
UNROLL = 8
SLOT = 33

EVERY = sorted(
    [
        (dx, dy, dz)
        for dx in range(NX) for dy in range(NY) for dz in range(NZ)
        if (dx, dy, dz) != (0, 0, 0)
    ],
    key=lambda o: -(min(o[0], NX - o[0]) + min(o[1], NY - o[1]) + min(o[2], NZ - o[2])),
)
OFFSETS = sorted(
    [(dy, dz) for dy in range(NY) for dz in range(NZ) if (dy, dz) != (0, 0)],
    key=lambda o: -(min(o[0], NY - o[0]) + min(o[1], NZ - o[1])),
)


def kernel(*args):
    pl.run_scoped(
        lambda *refs: work(refs[:-2], refs[-2:], *args),
        *([pltpu.ACC(0)((RB, 256), F32)] * (2 * FEAT // RB) + [pltpu.ACC(1)((FEAT, 256), F32)] * 2),
    )


def work(
    pieces, grad,
    x_hbm, w_hbm, b_hbm, t_hbm, m_hbm,
    out_o,
    xv, tv, mv, wi, wtmp, wg, wsq, wt, bi, wide,
    st_own, st_in, ab, cb, vb, sa, sc, acc, lacc, gt, sb, pin, ps, rr, nb,
    x_sem, t_sem, misc_sem,
    st_send, st_recv, w_send, w_recv, wp_send, wp_recv, c_send, c_recv, r_send, r_recv, b_send, b_recv,
):
    sets = (pieces[: FEAT // RB], pieces[FEAT // RB :])
    outs = (sa, sc)
    me = lax.axis_index("dp")
    mx = lax.axis_index("mp")
    core = lax.rem(me, NC)
    chip = lax.div(me, NC)
    my_y = lax.div(chip, NZ)
    my_z = lax.rem(chip, NZ)
    partner = me + 1 - 2 * core

    def chip_at(dy, dz):
        return lax.rem(my_y + dy, NY) * NZ + lax.rem(my_z + dz, NZ)

    w_copy = pltpu.make_async_copy(w_hbm, wi, misc_sem.at[0])
    w_copy.start()
    b_copy = pltpu.make_async_copy(b_hbm, bi, misc_sem.at[2])
    b_copy.start()

    barrier = pltpu.get_barrier_semaphore()
    for dy, dz in OFFSETS:
        for c in range(NC):
            pl.semaphore_signal(
                barrier, inc=1, device_id=(chip_at(dy, dz) * NC + c, mx), device_id_type=MESH
            )
    pl.semaphore_signal(barrier, inc=1, device_id=(partner, mx), device_id_type=MESH)
    for dx in range(1, NX):
        pl.semaphore_signal(
            barrier, inc=1, device_id=(me, lax.rem(mx + dx, NX)), device_id_type=MESH
        )

    def t_copy(g):
        return pltpu.make_async_copy(
            t_hbm.at[pl.ds(g * GI, GI)], tv.at[pl.ds(g * GI, GI)], t_sem.at[g]
        )

    def x_copy(g):
        return pltpu.make_async_copy(
            x_hbm.at[pl.ds(g * GI, GI)], xv.at[pl.ds(g * GI, GI), :, pl.ds(0, E)], x_sem.at[g]
        )

    def start_t(g, _):
        t_copy(g).start()
        return 0

    lax.fori_loop(0, NG, start_t, 0)
    m_copy = pltpu.make_async_copy(m_hbm, mv, misc_sem.at[1])
    m_copy.start()

    w_copy.wait()
    wide[...] = jnp.zeros_like(wide)
    wf = wi[...].astype(F32)
    wide[:, 0:FEAT] = wf
    half = ROWS // 2
    wtmp[2 * ROWS : 32, :] = jnp.zeros((32 - 2 * ROWS, 128), F32)
    wtmp[0:ROWS, :] = wide[:, 0:128]
    wtmp[ROWS : 2 * ROWS, :] = wide[:, 128:256]
    wtmp[2 * ROWS : 2 * ROWS + half, :] = wide[0:half, 256:384] + pltpu.roll(
        wide[half:ROWS, 256:384], 64, 1
    )
    wg[core, chip] = wtmp[...].astype(BF16)

    pl.semaphore_wait(barrier, (NCHIP - 1) * NC + NX)

    def w_dst(n):
        return pltpu.make_async_remote_copy(
            src_ref=wg.at[core, chip],
            dst_ref=wg.at[core, chip],
            send_sem=w_send,
            recv_sem=w_recv,
            device_id=(n * NC + core, mx),
            device_id_type=MESH,
        )

    for dy, dz in OFFSETS:
        w_dst(chip_at(dy, dz)).start()

    b_copy.wait()
    wsq[...] = jnp.zeros_like(wsq)
    b_all = bi[...].reshape(1, FEAT)
    b_high = b_all.astype(BF16).astype(F32)
    b_mid = (b_all - b_high).astype(BF16).astype(F32)
    wsq[E : E + 1, 0:FEAT] = b_high
    wsq[E + 1 : E + 2, 0:FEAT] = b_mid
    wsq[E + 2 : E + 3, 0:FEAT] = (b_all - b_high) - b_mid
    acc[...] = jnp.zeros_like(acc)
    lacc[...] = jnp.zeros_like(lacc)
    sc[...] = jnp.zeros_like(sc)
    none = jnp.zeros((RB, 256), BF16)
    for q in range(2):
        pltpu.matmul_acc_lhs(pieces[0], none, load_staged_rhs=q)
        pltpu.matmul_acc_lhs(grad[0], jnp.zeros((FEAT, 256), BF16), load_staged_rhs=q)
    for piece in (*pieces, *grad):
        pltpu.matmul_pop(piece)


    lane_x = lax.broadcasted_iota(jnp.int32, (1, 1, XW - E), 2)
    ones = jnp.where(lane_x < 3, 1.0, 0.0).astype(BF16)

    def stats(g):
        t_copy(g).wait()
        x_copy(g).start()
        xv[pl.ds(g * GI, GI), :, E:XW] = jnp.broadcast_to(ones, (GI, PAT, XW - E))
        sums, squares = [], []
        for k in range(GI):
            s8 = jnp.zeros((8, PAT), F32)
            q8 = jnp.zeros((8, PAT), F32)
            for r in range(0, FEAT, RB):
                t = tv[g * GI + k, r : r + RB, :].astype(F32).reshape(RB // 8, 8, PAT)
                s8 = s8 + jnp.sum(t, axis=0)
                q8 = q8 + jnp.sum(t * t, axis=0)
            sums.append(jnp.sum(s8, axis=0, keepdims=True))
            squares.append(jnp.sum(q8, axis=0, keepdims=True))
        st_own[g] = jnp.concatenate(sums + squares, axis=0)

    def st_copy(g, p):
        return pltpu.make_async_remote_copy(
            src_ref=st_own.at[g],
            dst_ref=st_in.at[p - 1, g],
            send_sem=st_send.at[p - 1, g],
            recv_sem=st_recv.at[p - 1, g],
            device_id=(me, lax.rem(mx + p, NX)),
            device_id_type=MESH,
        )

    def send_stats(g):
        for p in (2, 1, 3):
            st_copy(g, p).start()

    stats(0)

    def stats_and_send(g, _):
        stats(g)
        send_stats(g - 1)
        return 0

    lax.fori_loop(1, NG, stats_and_send, 0)

    m_copy.wait()

    def cover(i, total):
        v = jnp.sum(mv[i].astype(F32), axis=0, keepdims=True)
        vb[i] = jnp.broadcast_to(v, (8, PAT))
        return total + v

    counts = lax.fori_loop(0, IMG, cover, jnp.zeros((1, PAT), F32))
    send_stats(NG - 1)

    def prepare(g):
        for p in (1, 2, 3):
            st_copy(g, p).wait_recv()
        st = (st_own[g] + st_in[0, g]) + (st_in[1, g] + st_in[2, g])
        mean = st[0:GI] * (1.0 / FULL)
        var = jnp.maximum(st[GI : 2 * GI] * (1.0 / FULL) - mean * mean, 0.0)
        a = lax.rsqrt(var + 1e-05)
        c = mean * a
        for k in range(GI):
            ab[g * GI + k] = jnp.broadcast_to(a[k : k + 1], (8, PAT))
            cb[g * GI + k] = jnp.broadcast_to(c[k : k + 1], (8, PAT))

    def prepare_all(g, _):
        prepare(g)
        return 0

    lax.fori_loop(0, NG // 4, prepare_all, 0)

    whole = wg.at[0, pl.ds(0, NCHIP - 1)]
    pltpu.make_async_copy(whole, whole, w_recv).wait()
    w_pair = pltpu.make_async_remote_copy(
        src_ref=wg.at[core], dst_ref=wg.at[core], send_sem=wp_send, recv_sem=wp_recv,
        device_id=(partner, mx), device_id_type=MESH,
    )
    w_pair.start()
    w_pair.wait_recv()

    left = lax.broadcasted_iota(jnp.int32, (half, 128), 1) < 64
    for j in range(NDP):
        r = j * ROWS
        wtmp[...] = wg[j % NC, j // NC].astype(F32)
        wsq[r : r + ROWS, 0:128] = wtmp[0:ROWS, :]
        wsq[r : r + ROWS, 128:256] = wtmp[ROWS : 2 * ROWS, :]
        both = wtmp[2 * ROWS : 2 * ROWS + half, :]
        wsq[r : r + half, 256:384] = jnp.where(left, both, 0.0)
        wsq[r + half : r + ROWS, 256:384] = jnp.where(left, pltpu.roll(both, 64, 1), 0.0)
    wt[...] = jnp.transpose(wsq[...])[0:FEAT, :].astype(BF16)

    def first(i, pieces):
        for q in range(2):
            pltpu.matmul_push_rhs(
                xv[i, :, 256 * q : 256 * q + 256], staging_register=q, mxu_index=0, transpose=True
            )
        for q in range(2):
            for n, piece in enumerate(pieces):
                pltpu.matmul_acc_lhs(
                    piece, wt[RB * n : RB * n + RB, 256 * q : 256 * q + 256],
                    load_staged_rhs=q if n == 0 else None,
                )

    def second(i, source):
        for q in range(2):
            pltpu.matmul_push_rhs(
                xv[i, :, 256 * q : 256 * q + 256], staging_register=q, mxu_index=1
            )
        for q in range(2):
            pltpu.matmul_acc_lhs(grad[q], source[...], load_staged_rhs=q)

    def middle(i, pieces, target):
        a = ab[i][None]
        c = cb[i][None]
        v = vb[i][None]
        loss8 = jnp.zeros((8, PAT), F32)
        for n, piece in enumerate(pieces):
            r = RB * n
            p = pltpu.matmul_pop(piece).reshape(RB // 8, 8, PAT)
            t = tv[i, r : r + RB, :].astype(F32).reshape(RB // 8, 8, PAT)
            d = p - (t * a - c)
            h = jnp.minimum(jnp.maximum(d, -1.0), 1.0)
            s = v * h
            loss8 = loss8 + jnp.sum(s * (d - 0.5 * h), axis=0)
            s = s.reshape(RB, PAT)
            target[r : r + RB, :] = s.astype(BF16)
            acc[r : r + RB, E : E + 128] += s[:, 0:128] + s[:, 128:256]
        lacc[...] += loss8

    def x_here(g, _):
        x_copy(g).wait()
        return 0

    lax.fori_loop(0, NG, x_here, 0)
    first(0, sets[0])

    def main(g, _):
        base = g * UNROLL
        for u in range(UNROLL):
            first(jnp.minimum(base + u + 1, IMG - 1), sets[(u + 1) % 2])
            second(jnp.maximum(base + u - 1, 0), outs[(u + 1) % 2])
            middle(base + u, sets[u % 2], outs[u % 2])
        return 0

    trips = IMG // UNROLL
    lax.fori_loop(0, trips // 4, main, 0)
    lax.fori_loop(NG // 4, NG, prepare_all, 0)
    lax.fori_loop(trips // 4, trips, main, 0)
    second(IMG - 1, outs[1])
    acc[0:FEAT, 0:256] = pltpu.matmul_pop(grad[0])
    acc[0:FEAT, 256:E] = pltpu.matmul_pop(grad[1])[:, 0:128]
    for piece in sets[0]:
        pltpu.matmul_pop(piece)

    gt[...] = jnp.transpose(acc[...])
    gb = jnp.sum(gt[E : E + 128, :], axis=0, keepdims=True)
    loss_all = jnp.sum(lacc[...])
    count_all = jnp.sum(counts)
    lane = lax.broadcasted_iota(jnp.int32, (1, 128), 1)
    tail = jnp.where(lane < 64, gb[:, 256:384], jnp.where(lane < 96, loss_all, count_all))
    for j in range(NDP):
        r = j * ROWS
        slot = sb.at[j % NC, j // NC]
        slot[0:ROWS, :] = gt[r : r + ROWS, 0:128]
        slot[ROWS : 2 * ROWS, :] = gt[r : r + ROWS, 128:256]
        half = ROWS // 2
        up = gt[r : r + half, 256:384]
        down = gt[r + half : r + ROWS, 256:384]
        slot[2 * ROWS : 2 * ROWS + half, :] = up + pltpu.roll(down, 64, 1)
        slot[30:31, :] = gb[:, 0:128]
        slot[31:32, :] = gb[:, 128:256]
        slot[32:33, :] = tail

    order = [chip_at(dy, dz) for dy, dz in OFFSETS] + [chip]

    def pair(k):
        n = order[k]
        return pltpu.make_async_remote_copy(
            src_ref=sb.at[1 - core, n, pl.ds(0, SLOT)], dst_ref=pin.at[n, pl.ds(0, SLOT)],
            send_sem=c_send.at[k], recv_sem=c_recv.at[k],
            device_id=(partner, mx), device_id_type=MESH,
        )

    def r_copy(n):
        return pltpu.make_async_remote_copy(
            src_ref=ps.at[n, pl.ds(0, SLOT)], dst_ref=rr.at[chip, pl.ds(0, SLOT)],
            send_sem=r_send, recv_sem=r_recv,
            device_id=(n * NC + core, mx), device_id_type=MESH,
        )

    for k in range(NCHIP):
        pair(k).start()
    for k in range(NCHIP):
        n = order[k]
        pair(k).wait_recv()
        both = sb[core, n, 0:SLOT] + pin[n, 0:SLOT]
        if k < NCHIP - 1:
            ps[n, 0:SLOT] = both
        else:
            rr[n, 0:SLOT] = both
        if k > 0:
            r_copy(order[k - 1]).start()
    others = rr.at[pl.ds(0, NCHIP - 1), pl.ds(0, SLOT)]
    pltpu.make_async_copy(others, others, r_recv).wait()
    mine = jnp.sum(rr[:, 0:SLOT], axis=0)
    gbl = mine[30:33]
    lane3 = lax.broadcasted_iota(jnp.int32, (3, 128), 1)
    row3 = lax.broadcasted_iota(jnp.int32, (3, 128), 0)
    gbz = jnp.where((row3 < 2) | (lane3 < 64), gbl, 0.0)
    square = jnp.sum(mine[0:30] * mine[0:30]) + jnp.sum(gbz * gbz) * (1.0 / NDP)
    lrow = mine[32:33, :]
    loss_plane = jnp.sum(jnp.where(lane == 64, lrow, 0.0))
    count = jnp.sum(jnp.where(lane == 96, lrow, 0.0))
    ident = me * NX + mx
    nb[ident] = jnp.where(lane < 64, square, loss_plane)

    def b_out(n, m):
        return pltpu.make_async_remote_copy(
            src_ref=nb.at[ident], dst_ref=nb.at[ident], send_sem=b_send, recv_sem=b_recv,
            device_id=(n, m), device_id_type=MESH,
        )

    for dx, dy, dz in EVERY:
        for c in range(NC):
            b_out(chip_at(dy, dz) * NC + c, lax.rem(mx + dx, NX)).start()
    b_out(partner, mx).start()
    rest_b = nb.at[pl.ds(0, NDP * NX - 1)]
    pltpu.make_async_copy(rest_b, rest_b, b_recv).wait()
    parts = [jnp.sum(nb[16 * q : 16 * q + 16], axis=0) for q in range(NDP * NX // 16)]
    final = ((parts[0] + parts[1]) + (parts[2] + parts[3])) + (
        (parts[4] + parts[5]) + (parts[6] + parts[7])
    )
    loss_sum = jnp.sum(jnp.where(lane == 64, final, 0.0)) * (1.0 / NDP)
    total = jnp.broadcast_to(final[0:1, 0:1], (1, 128))
    countv = jnp.full((1, 128), count, F32)
    norm = jnp.sqrt(total) / countv
    clip = jnp.minimum(1.0, 1.0 / (norm + 1e-06))
    factor = clip / countv
    loss = jnp.full((1, 128), loss_sum, F32) / countv * (1.0 / FULL)
    out_o[0:SLOT] = mine * factor
    out_o[SLOT : SLOT + 1] = loss
    out_o[SLOT + 1 : SLOT + 2] = clip
    out_o[SLOT + 2 :] = jnp.zeros((40 - SLOT - 2, 128), F32)

    def drain(g, _):
        for p in (1, 2, 3):
            st_copy(g, p).wait_send()
        return 0

    lax.fori_loop(0, NG, drain, 0)
    pltpu.make_async_copy(whole, whole, w_send).wait()
    w_pair.wait_send()
    for k in range(NCHIP):
        pair(k).wait_send()
    sent = ps.at[pl.ds(0, NCHIP - 1), pl.ds(0, SLOT)]
    pltpu.make_async_copy(sent, sent, r_send).wait()
    pltpu.make_async_copy(rest_b, rest_b, b_send).wait()


def spread(in_ref, loss_o, clip_o, gw_o, gb_o):
    half = ROWS // 2
    gw_o[:, 0:128] = in_ref[0:ROWS]
    gw_o[:, 128:256] = in_ref[ROWS : 2 * ROWS]
    gw_o[0:half, 256:320] = in_ref[2 * ROWS : 2 * ROWS + half, 0:64]
    gw_o[half:ROWS, 256:320] = in_ref[2 * ROWS : 2 * ROWS + half, 64:128]
    gb_o[...] = jnp.concatenate(
        [in_ref[30:31, :], in_ref[31:32, :], in_ref[32:33, 0:64]], axis=1
    ).reshape(FEAT)
    loss_o[...] = in_ref[33:34, 0:1]
    clip_o[...] = in_ref[34:35, 0:1]


def body(pred_input, proj_weight, proj_bias, targets, block_masks):
    any_spec = pl.BlockSpec(memory_space=pl.ANY)
    vmem_spec = pl.BlockSpec(memory_space=pltpu.VMEM)
    vm = pltpu.VMEM
    dma = pltpu.SemaphoreType.DMA
    packed = pl.pallas_call(
        kernel,
        name="fused",
        out_shape=jax.ShapeDtypeStruct((40, 128), F32),
        in_specs=[any_spec] * 5,
        out_specs=vmem_spec,
        scratch_shapes=[
            vm((IMG, PAT, XW), BF16),
            vm((IMG, FEAT, PAT), BF16),
            vm((IMG, 4, PAT), jnp.int32),
            vm((ROWS, FEAT), BF16),
            vm((32, 128), F32),
            vm((NC, NCHIP, 32, 128), BF16),
            vm((XW, FP), F32),
            vm((FEAT, XW), BF16),
            vm((FEAT,), F32),
            vm((ROWS, FP), F32),
            vm((NG, 2 * GI, PAT), F32),
            vm((NX - 1, NG, 2 * GI, PAT), F32),
            vm((IMG, 8, PAT), F32),
            vm((IMG, 8, PAT), F32),
            vm((IMG, 8, PAT), F32),
            vm((FEAT, PAT), BF16),
            vm((FEAT, PAT), BF16),
            vm((FP, E + 128), F32),
            vm((8, PAT), F32),
            vm((E + 128, FP), F32),
            vm((NC, NCHIP, 40, 128), F32),
            vm((NCHIP, 40, 128), F32),
            vm((NCHIP, 40, 128), F32),
            vm((NCHIP, 40, 128), F32),
            vm((NDP * NX, 1, 128), F32),
            dma((NG,)), dma((NG,)), dma((3,)),
            dma((NX - 1, NG)), dma((NX - 1, NG)),
            dma, dma, dma, dma, dma((NCHIP,)), dma((NCHIP,)), dma, dma, dma, dma,
        ],
        compiler_params=pltpu.CompilerParams(
            collective_id=0, has_side_effects=True, vmem_limit_bytes=64 * 1024 * 1024 - 65536,
        ),
    )(
        pred_input,
        proj_weight,
        proj_bias,
        jnp.swapaxes(targets, 1, 2),
        block_masks,
    )
    loss, clip, gw, gb = pl.pallas_call(
        spread,
        name="spread",
        out_shape=(
            jax.ShapeDtypeStruct((1, 1), F32),
            jax.ShapeDtypeStruct((1, 1), F32),
            jax.ShapeDtypeStruct((ROWS, FEAT), F32),
            jax.ShapeDtypeStruct((FEAT,), F32),
        ),
        in_specs=[vmem_spec],
        out_specs=(vmem_spec,) * 4,
    )(packed)
    return loss.reshape(()), clip.reshape(()), gw, gb


def solution(mesh):
    return jax.shard_map(
        body,
        mesh=mesh,
        in_specs=(
            P("dp", None, None), P("dp", "mp"), P("mp"), P("dp", None, "mp"), P("dp", None, None),
        ),
        out_specs=(P(), P(), P("dp", "mp"), P("mp")),
        check_vma=False,
    )
```

```python
import jax
import jax.numpy as jnp
from jax import lax
from jax.experimental import pallas as pl
from jax.experimental.pallas import tpu as pltpu
from jax.sharding import PartitionSpec as P

MESH = pl.DeviceIdType.MESH
F32 = jnp.float32
BF16 = jnp.bfloat16

NY, NZ, NC, NX = 4, 4, 2, 4
NCHIP = NY * NZ
NDP = NCHIP * NC
GI = 4
NG = 16
IMG = GI * NG
PAT = 256
FEAT = 320
FULL = FEAT * NX
E = 384
ROWS = E // NDP
FP = 384
RB = 64
XW = 512
UNROLL = 16
SLOT = 33

EVERY = sorted(
    [
        (dx, dy, dz)
        for dx in range(NX) for dy in range(NY) for dz in range(NZ)
        if (dx, dy, dz) != (0, 0, 0)
    ],
    key=lambda o: -(min(o[0], NX - o[0]) + min(o[1], NY - o[1]) + min(o[2], NZ - o[2])),
)
OFFSETS = sorted(
    [(dy, dz) for dy in range(NY) for dz in range(NZ) if (dy, dz) != (0, 0)],
    key=lambda o: -(min(o[0], NY - o[0]) + min(o[1], NZ - o[1])),
)


def kernel(*args):
    pl.run_scoped(
        lambda *refs: work(refs[:-2], refs[-2:], *args),
        *([pltpu.ACC(0)((RB, 256), F32)] * (2 * FEAT // RB) + [pltpu.ACC(1)((FEAT, 256), F32)] * 2),
    )


def work(
    pieces, grad,
    x_hbm, w_hbm, b_hbm, t_hbm, m_hbm,
    out_o,
    xv, tv, mv, wi, wtmp, wf32, wg, wsq, wt, bi, wide,
    st_own, st_in, ab, cb, vb, sa, sc, acc, lacc, gt, sb, pin, ps, rr, nb,
    x_sem, t_sem, misc_sem,
    st_send, st_recv, w_send, w_recv, wp_send, wp_recv, c_send, c_recv, r_send, r_recv, b_send, b_recv,
):
    sets = (pieces[: FEAT // RB], pieces[FEAT // RB :])
    outs = (sa, sc)
    me = lax.axis_index("dp")
    mx = lax.axis_index("mp")
    core = lax.rem(me, NC)
    chip = lax.div(me, NC)
    my_y = lax.div(chip, NZ)
    my_z = lax.rem(chip, NZ)
    partner = me + 1 - 2 * core

    def chip_at(dy, dz):
        return lax.rem(my_y + dy, NY) * NZ + lax.rem(my_z + dz, NZ)

    w_copy = pltpu.make_async_copy(w_hbm, wi, misc_sem.at[0])
    w_copy.start()
    b_copy = pltpu.make_async_copy(b_hbm, bi, misc_sem.at[2])
    b_copy.start()

    barrier = pltpu.get_barrier_semaphore()
    for dy, dz in OFFSETS:
        for c in range(NC):
            pl.semaphore_signal(
                barrier, inc=1, device_id=(chip_at(dy, dz) * NC + c, mx), device_id_type=MESH
            )
    pl.semaphore_signal(barrier, inc=1, device_id=(partner, mx), device_id_type=MESH)
    for dx in range(1, NX):
        pl.semaphore_signal(
            barrier, inc=1, device_id=(me, lax.rem(mx + dx, NX)), device_id_type=MESH
        )

    def t_copy(g):
        return pltpu.make_async_copy(
            t_hbm.at[pl.ds(g * GI, GI)], tv.at[pl.ds(g * GI, GI)], t_sem.at[g]
        )

    def x_copy(g):
        return pltpu.make_async_copy(
            x_hbm.at[pl.ds(g * GI, GI)], xv.at[pl.ds(g * GI, GI), :, pl.ds(0, E)], x_sem.at[g]
        )

    def start_t(g, _):
        t_copy(g).start()
        return 0

    lax.fori_loop(0, NG, start_t, 0)
    m_copy = pltpu.make_async_copy(m_hbm, mv, misc_sem.at[1])
    m_copy.start()

    w_copy.wait()
    wide[...] = jnp.zeros_like(wide)
    wf = wi[...].astype(F32)
    wide[:, 0:FEAT] = wf
    half = ROWS // 2
    wtmp[2 * ROWS : 32, :] = jnp.zeros((32 - 2 * ROWS, 128), F32)
    wtmp[0:ROWS, :] = wide[:, 0:128]
    wtmp[ROWS : 2 * ROWS, :] = wide[:, 128:256]
    wtmp[2 * ROWS : 2 * ROWS + half, :] = wide[0:half, 256:384] + pltpu.roll(
        wide[half:ROWS, 256:384], 64, 1
    )
    wg[core, chip] = wtmp[...].astype(BF16)

    pl.semaphore_wait(barrier, (NCHIP - 1) * NC + NX)

    def w_dst(n):
        return pltpu.make_async_remote_copy(
            src_ref=wg.at[core, chip],
            dst_ref=wg.at[core, chip],
            send_sem=w_send,
            recv_sem=w_recv,
            device_id=(n * NC + core, mx),
            device_id_type=MESH,
        )

    for dy, dz in OFFSETS:
        w_dst(chip_at(dy, dz)).start()

    b_copy.wait()
    wsq[...] = jnp.zeros_like(wsq)
    b_all = bi[...].reshape(1, FEAT)
    b_high = b_all.astype(BF16).astype(F32)
    b_mid = (b_all - b_high).astype(BF16).astype(F32)
    wsq[E : E + 1, 0:FEAT] = b_high
    wsq[E + 1 : E + 2, 0:FEAT] = b_mid
    wsq[E + 2 : E + 3, 0:FEAT] = (b_all - b_high) - b_mid
    acc[...] = jnp.zeros_like(acc)
    lacc[...] = jnp.zeros_like(lacc)
    sc[...] = jnp.zeros_like(sc)
    none = jnp.zeros((RB, 256), BF16)
    for q in range(2):
        pltpu.matmul_acc_lhs(pieces[0], none, load_staged_rhs=q)
        pltpu.matmul_acc_lhs(grad[0], jnp.zeros((FEAT, 256), BF16), load_staged_rhs=q)
    for piece in (*pieces, *grad):
        pltpu.matmul_pop(piece)


    lane_x = lax.broadcasted_iota(jnp.int32, (1, 1, XW - E), 2)
    ones = jnp.where(lane_x < 3, 1.0, 0.0).astype(BF16)

    def stats(g):
        t_copy(g).wait()
        x_copy(g).start()
        xv[pl.ds(g * GI, GI), :, E:XW] = jnp.broadcast_to(ones, (GI, PAT, XW - E))
        sums, squares = [], []
        for k in range(GI):
            s8 = jnp.zeros((8, PAT), F32)
            q8 = jnp.zeros((8, PAT), F32)
            for r in range(0, FEAT, RB):
                t = tv[g * GI + k, r : r + RB, :].astype(F32).reshape(RB // 8, 8, PAT)
                s8 = s8 + jnp.sum(t, axis=0)
                q8 = q8 + jnp.sum(t * t, axis=0)
            sums.append(jnp.sum(s8, axis=0, keepdims=True))
            squares.append(jnp.sum(q8, axis=0, keepdims=True))
        st_own[g] = jnp.concatenate(sums + squares, axis=0)

    def st_copy(g, p):
        return pltpu.make_async_remote_copy(
            src_ref=st_own.at[g],
            dst_ref=st_in.at[p - 1, g],
            send_sem=st_send.at[p - 1, g],
            recv_sem=st_recv.at[p - 1, g],
            device_id=(me, lax.rem(mx + p, NX)),
            device_id_type=MESH,
        )

    def send_stats(g):
        for p in (2, 1, 3):
            st_copy(g, p).start()

    stats(0)

    def stats_and_send(g, _):
        stats(g)
        send_stats(g - 1)
        return 0

    lax.fori_loop(1, NG, stats_and_send, 0)

    m_copy.wait()

    def cover(i, total):
        v = jnp.sum(mv[i].astype(F32), axis=0, keepdims=True)
        vb[i] = jnp.broadcast_to(v, (8, PAT))
        return total + v

    counts = lax.fori_loop(0, IMG, cover, jnp.zeros((1, PAT), F32))
    send_stats(NG - 1)

    def prepare(g):
        for p in (1, 2, 3):
            st_copy(g, p).wait_recv()
        st = (st_own[g] + st_in[0, g]) + (st_in[1, g] + st_in[2, g])
        mean = st[0:GI] * (1.0 / FULL)
        var = jnp.maximum(st[GI : 2 * GI] * (1.0 / FULL) - mean * mean, 0.0)
        a = lax.rsqrt(var + 1e-05)
        c = mean * a
        for k in range(GI):
            ab[g * GI + k] = jnp.broadcast_to(a[k : k + 1], (8, PAT))
            cb[g * GI + k] = jnp.broadcast_to(c[k : k + 1], (8, PAT))

    whole = wg.at[0, pl.ds(0, NCHIP - 1)]
    pltpu.make_async_copy(whole, whole, w_recv).wait()
    w_pair = pltpu.make_async_remote_copy(
        src_ref=wg.at[core], dst_ref=wg.at[core], send_sem=wp_send, recv_sem=wp_recv,
        device_id=(partner, mx), device_id_type=MESH,
    )
    w_pair.start()

    def prepare_all(g, _):
        prepare(g)
        return 0

    lax.fori_loop(0, NG // 4, prepare_all, 0)

    w_pair.wait_recv()

    left = lax.broadcasted_iota(jnp.int32, (half, 128), 1) < 64
    for j in range(NDP):
        r = j * ROWS
        wf32[j] = wg[j % NC, j // NC].astype(F32)
        wsq[r : r + ROWS, 0:128] = wf32[j, 0:ROWS]
        wsq[r : r + ROWS, 128:256] = wf32[j, ROWS : 2 * ROWS]
        both = wf32[j, 2 * ROWS : 2 * ROWS + half]
        wsq[r : r + half, 256:384] = jnp.where(left, both, 0.0)
        wsq[r + half : r + ROWS, 256:384] = jnp.where(left, pltpu.roll(both, 64, 1), 0.0)
    wt[...] = jnp.transpose(wsq[...])[0:FEAT, :].astype(BF16)

    def first(i, pieces):
        for q in range(2):
            pltpu.matmul_push_rhs(
                xv[i, :, 256 * q : 256 * q + 256], staging_register=q, mxu_index=0, transpose=True
            )
        for q in range(2):
            for n, piece in enumerate(pieces):
                pltpu.matmul_acc_lhs(
                    piece, wt[RB * n : RB * n + RB, 256 * q : 256 * q + 256],
                    load_staged_rhs=q if n == 0 else None,
                )

    def second(i, source):
        for q in range(2):
            pltpu.matmul_push_rhs(
                xv[i, :, 256 * q : 256 * q + 256], staging_register=q, mxu_index=1
            )
        for q in range(2):
            pltpu.matmul_acc_lhs(grad[q], source[...], load_staged_rhs=q)

    def middle(i, pieces, target):
        a = ab[i][None]
        c = cb[i][None]
        v = vb[i][None]
        loss8 = jnp.zeros((8, PAT), F32)
        for n, piece in enumerate(pieces):
            r = RB * n
            p = pltpu.matmul_pop(piece).reshape(RB // 8, 8, PAT)
            t = tv[i, r : r + RB, :].astype(F32).reshape(RB // 8, 8, PAT)
            d = p - (t * a - c)
            h = jnp.minimum(jnp.maximum(d, -1.0), 1.0)
            s = v * h
            loss8 = loss8 + jnp.sum(s * (d - 0.5 * h), axis=0)
            s = s.reshape(RB, PAT)
            target[r : r + RB, :] = s.astype(BF16)
            acc[r : r + RB, E : E + 128] += s[:, 0:128] + s[:, 128:256]
        lacc[...] += loss8

    def x_here(g, _):
        x_copy(g).wait()
        return 0

    lax.fori_loop(0, NG, x_here, 0)
    first(0, sets[0])

    def main(g, _):
        base = g * UNROLL
        for u in range(UNROLL):
            first(jnp.minimum(base + u + 1, IMG - 1), sets[(u + 1) % 2])
            second(jnp.maximum(base + u - 1, 0), outs[(u + 1) % 2])
            middle(base + u, sets[u % 2], outs[u % 2])
        return 0

    trips = IMG // UNROLL
    lax.fori_loop(0, trips // 4, main, 0)
    lax.fori_loop(NG // 4, NG, prepare_all, 0)
    lax.fori_loop(trips // 4, trips, main, 0)
    second(IMG - 1, outs[1])
    acc[0:FEAT, 0:256] = pltpu.matmul_pop(grad[0])
    acc[0:FEAT, 256:E] = pltpu.matmul_pop(grad[1])[:, 0:128]
    for piece in sets[0]:
        pltpu.matmul_pop(piece)

    gt[...] = jnp.transpose(acc[...])
    gb = jnp.sum(gt[E : E + 128, :], axis=0, keepdims=True)
    loss_all = jnp.sum(lacc[...])
    count_all = jnp.sum(counts)
    lane = lax.broadcasted_iota(jnp.int32, (1, 128), 1)
    tail = jnp.where(lane < 64, gb[:, 256:384], jnp.where(lane < 96, loss_all, count_all))
    for j in range(NDP):
        r = j * ROWS
        slot = sb.at[j % NC, j // NC]
        slot[0:ROWS, :] = gt[r : r + ROWS, 0:128]
        slot[ROWS : 2 * ROWS, :] = gt[r : r + ROWS, 128:256]
        half = ROWS // 2
        up = gt[r : r + half, 256:384]
        down = gt[r + half : r + ROWS, 256:384]
        slot[2 * ROWS : 2 * ROWS + half, :] = up + pltpu.roll(down, 64, 1)
        slot[30:31, :] = gb[:, 0:128]
        slot[31:32, :] = gb[:, 128:256]
        slot[32:33, :] = tail

    order = [chip_at(dy, dz) for dy, dz in OFFSETS] + [chip]

    def pair(k):
        n = order[k]
        return pltpu.make_async_remote_copy(
            src_ref=sb.at[1 - core, n, pl.ds(0, SLOT)], dst_ref=pin.at[n, pl.ds(0, SLOT)],
            send_sem=c_send.at[k], recv_sem=c_recv.at[k],
            device_id=(partner, mx), device_id_type=MESH,
        )

    def r_copy(n):
        return pltpu.make_async_remote_copy(
            src_ref=ps.at[n, pl.ds(0, SLOT)], dst_ref=rr.at[chip, pl.ds(0, SLOT)],
            send_sem=r_send, recv_sem=r_recv,
            device_id=(n * NC + core, mx), device_id_type=MESH,
        )

    for k in range(NCHIP):
        pair(k).start()
    for k in range(NCHIP):
        n = order[k]
        pair(k).wait_recv()
        both = sb[core, n, 0:SLOT] + pin[n, 0:SLOT]
        if k < NCHIP - 1:
            ps[n, 0:SLOT] = both
        else:
            rr[n, 0:SLOT] = both
        if k > 0:
            r_copy(order[k - 1]).start()
    others = rr.at[pl.ds(0, NCHIP - 1), pl.ds(0, SLOT)]
    pltpu.make_async_copy(others, others, r_recv).wait()
    mine = jnp.sum(rr[:, 0:SLOT], axis=0)
    gbl = mine[30:33]
    lane3 = lax.broadcasted_iota(jnp.int32, (3, 128), 1)
    row3 = lax.broadcasted_iota(jnp.int32, (3, 128), 0)
    gbz = jnp.where((row3 < 2) | (lane3 < 64), gbl, 0.0)
    squares = jnp.sum(mine[0:30] * mine[0:30], axis=0, keepdims=True) + jnp.sum(
        gbz * gbz, axis=0, keepdims=True
    ) * (1.0 / NDP)
    lrow = mine[32:33, :]
    ident = me * NX + mx
    nb[ident, 0:1] = squares
    nb[ident, 1:2] = lrow

    def b_out(n, m):
        return pltpu.make_async_remote_copy(
            src_ref=nb.at[ident], dst_ref=nb.at[ident], send_sem=b_send, recv_sem=b_recv,
            device_id=(n, m), device_id_type=MESH,
        )

    for dx, dy, dz in EVERY:
        for c in range(NC):
            b_out(chip_at(dy, dz) * NC + c, lax.rem(mx + dx, NX)).start()
    b_out(partner, mx).start()
    rest_b = nb.at[pl.ds(0, NDP * NX - 1)]
    def drain(g, _):
        for p in (1, 2, 3):
            st_copy(g, p).wait_send()
        return 0

    lax.fori_loop(0, NG, drain, 0)
    pltpu.make_async_copy(whole, whole, w_send).wait()
    w_pair.wait_send()
    for k in range(NCHIP):
        pair(k).wait_send()
    sent = ps.at[pl.ds(0, NCHIP - 1), pl.ds(0, SLOT)]
    pltpu.make_async_copy(sent, sent, r_send).wait()
    pltpu.make_async_copy(rest_b, rest_b, b_recv).wait()
    parts = [jnp.sum(nb[16 * q : 16 * q + 16], axis=0) for q in range(NDP * NX // 16)]
    final = ((parts[0] + parts[1]) + (parts[2] + parts[3])) + (
        (parts[4] + parts[5]) + (parts[6] + parts[7])
    )
    loss_sum = jnp.sum(jnp.where(lane == 64, final[1:2], 0.0)) * (1.0 / NDP)
    count = jnp.sum(jnp.where(lane == 96, lrow, 0.0))
    total = jnp.full((1, 128), jnp.sum(final[0:1]), F32)
    countv = jnp.full((1, 128), count, F32)
    norm = jnp.sqrt(total) / countv
    clip = jnp.minimum(1.0, 1.0 / (norm + 1e-06))
    factor = clip / countv
    loss = jnp.full((1, 128), loss_sum, F32) / countv * (1.0 / FULL)
    out_o[0:SLOT] = mine * factor
    out_o[SLOT : SLOT + 1] = loss
    out_o[SLOT + 1 : SLOT + 2] = clip
    out_o[SLOT + 2 :] = jnp.zeros((40 - SLOT - 2, 128), F32)
    pltpu.make_async_copy(rest_b, rest_b, b_send).wait()


def spread(in_ref, loss_o, clip_o, gw_o, gb_o):
    half = ROWS // 2
    gw_o[:, 0:128] = in_ref[0:ROWS]
    gw_o[:, 128:256] = in_ref[ROWS : 2 * ROWS]
    gw_o[0:half, 256:320] = in_ref[2 * ROWS : 2 * ROWS + half, 0:64]
    gw_o[half:ROWS, 256:320] = in_ref[2 * ROWS : 2 * ROWS + half, 64:128]
    gb_o[...] = jnp.concatenate(
        [in_ref[30:31, :], in_ref[31:32, :], in_ref[32:33, 0:64]], axis=1
    ).reshape(FEAT)
    loss_o[...] = in_ref[33:34, 0:1]
    clip_o[...] = in_ref[34:35, 0:1]


def body(pred_input, proj_weight, proj_bias, targets, block_masks):
    any_spec = pl.BlockSpec(memory_space=pl.ANY)
    vmem_spec = pl.BlockSpec(memory_space=pltpu.VMEM)
    vm = pltpu.VMEM
    dma = pltpu.SemaphoreType.DMA
    packed = pl.pallas_call(
        kernel,
        name="fused",
        out_shape=jax.ShapeDtypeStruct((40, 128), F32),
        in_specs=[any_spec] * 5,
        out_specs=vmem_spec,
        scratch_shapes=[
            vm((IMG, PAT, XW), BF16),
            vm((IMG, FEAT, PAT), BF16),
            vm((IMG, 4, PAT), jnp.int32),
            vm((ROWS, FEAT), BF16),
            vm((32, 128), F32),
            vm((NDP, 32, 128), F32),
            vm((NC, NCHIP, 32, 128), BF16),
            vm((XW, FP), F32),
            vm((FEAT, XW), BF16),
            vm((FEAT,), F32),
            vm((ROWS, FP), F32),
            vm((NG, 2 * GI, PAT), F32),
            vm((NX - 1, NG, 2 * GI, PAT), F32),
            vm((IMG, 8, PAT), F32),
            vm((IMG, 8, PAT), F32),
            vm((IMG, 8, PAT), F32),
            vm((FEAT, PAT), BF16),
            vm((FEAT, PAT), BF16),
            vm((FP, E + 128), F32),
            vm((8, PAT), F32),
            vm((E + 128, FP), F32),
            vm((NC, NCHIP, 40, 128), F32),
            vm((NCHIP, 40, 128), F32),
            vm((NCHIP, 40, 128), F32),
            vm((NCHIP, 40, 128), F32),
            vm((NDP * NX, 2, 128), F32),
            dma((NG,)), dma((NG,)), dma((3,)),
            dma((NX - 1, NG)), dma((NX - 1, NG)),
            dma, dma, dma, dma, dma((NCHIP,)), dma((NCHIP,)), dma, dma, dma, dma,
        ],
        compiler_params=pltpu.CompilerParams(
            collective_id=0, has_side_effects=True, vmem_limit_bytes=64 * 1024 * 1024 - 65536,
        ),
    )(
        pred_input,
        proj_weight,
        proj_bias,
        jnp.swapaxes(targets, 1, 2),
        block_masks,
    )
    loss, clip, gw, gb = pl.pallas_call(
        spread,
        name="spread",
        out_shape=(
            jax.ShapeDtypeStruct((1, 1), F32),
            jax.ShapeDtypeStruct((1, 1), F32),
            jax.ShapeDtypeStruct((ROWS, FEAT), F32),
            jax.ShapeDtypeStruct((FEAT,), F32),
        ),
        in_specs=[vmem_spec],
        out_specs=(vmem_spec,) * 4,
    )(packed)
    return loss.reshape(()), clip.reshape(()), gw, gb


def solution(mesh):
    return jax.shard_map(
        body,
        mesh=mesh,
        in_specs=(
            P("dp", None, None), P("dp", "mp"), P("mp"), P("dp", None, "mp"), P("dp", None, None),
        ),
        out_specs=(P(), P(), P("dp", "mp"), P("mp")),
        check_vma=False,
    )
```

```python
import jax
import jax.numpy as jnp
from jax import lax
from jax.experimental import pallas as pl
from jax.experimental.pallas import tpu as pltpu
from jax.sharding import PartitionSpec as P

MESH = pl.DeviceIdType.MESH
F32 = jnp.float32
BF16 = jnp.bfloat16

NY, NZ, NC, NX = 4, 4, 2, 4
NCHIP = NY * NZ
NDP = NCHIP * NC
GI = 4
NG = 16
IMG = GI * NG
PAT = 256
FEAT = 320
FULL = FEAT * NX
E = 384
ROWS = E // NDP
FP = 384
RB = 64
XW = 512
UNROLL = 16
SLOT = 33

EVERY = sorted(
    [
        (dx, dy, dz)
        for dx in range(NX) for dy in range(NY) for dz in range(NZ)
        if (dx, dy, dz) != (0, 0, 0)
    ],
    key=lambda o: -(min(o[0], NX - o[0]) + min(o[1], NY - o[1]) + min(o[2], NZ - o[2])),
)
OFFSETS = sorted(
    [(dy, dz) for dy in range(NY) for dz in range(NZ) if (dy, dz) != (0, 0)],
    key=lambda o: -(min(o[0], NY - o[0]) + min(o[1], NZ - o[1])),
)


def kernel(*args):
    pl.run_scoped(
        lambda *refs: work(refs[:-2], refs[-2:], *args),
        *([pltpu.ACC(0)((RB, 256), F32)] * (2 * FEAT // RB) + [pltpu.ACC(1)((FEAT, 256), F32)] * 2),
    )


def work(
    pieces, grad,
    x_hbm, w_hbm, b_hbm, t_hbm, m_hbm,
    out_o,
    xv, tv, mv, wi, wtmp, wf32, wg, wsq, wt, bi, wide,
    st_own, st_in, ab, cb, vb, sa, sc, acc, lacc, gt, sb, pin, ps, rr, nb,
    x_sem, t_sem, misc_sem,
    st_send, st_recv, w_send, w_recv, wp_send, wp_recv, c_send, c_recv, r_send, r_recv, b_send, b_recv,
):
    sets = (pieces[: FEAT // RB], pieces[FEAT // RB :])
    outs = (sa, sc)
    me = lax.axis_index("dp")
    mx = lax.axis_index("mp")
    core = lax.rem(me, NC)
    chip = lax.div(me, NC)
    my_y = lax.div(chip, NZ)
    my_z = lax.rem(chip, NZ)
    partner = me + 1 - 2 * core

    def chip_at(dy, dz):
        return lax.rem(my_y + dy, NY) * NZ + lax.rem(my_z + dz, NZ)

    w_copy = pltpu.make_async_copy(w_hbm, wi, misc_sem.at[0])
    w_copy.start()
    b_copy = pltpu.make_async_copy(b_hbm, bi, misc_sem.at[2])
    b_copy.start()

    barrier = pltpu.get_barrier_semaphore()
    for dy, dz in OFFSETS:
        for c in range(NC):
            pl.semaphore_signal(
                barrier, inc=1, device_id=(chip_at(dy, dz) * NC + c, mx), device_id_type=MESH
            )
    pl.semaphore_signal(barrier, inc=1, device_id=(partner, mx), device_id_type=MESH)
    for dx in range(1, NX):
        pl.semaphore_signal(
            barrier, inc=1, device_id=(me, lax.rem(mx + dx, NX)), device_id_type=MESH
        )

    def t_copy(g):
        return pltpu.make_async_copy(
            t_hbm.at[pl.ds(g * GI, GI)], tv.at[pl.ds(g * GI, GI)], t_sem.at[g]
        )

    def x_copy(g):
        return pltpu.make_async_copy(
            x_hbm.at[pl.ds(g * GI, GI)], xv.at[pl.ds(g * GI, GI), :, pl.ds(0, E)], x_sem.at[g]
        )

    def start_t(g, _):
        t_copy(g).start()
        return 0

    lax.fori_loop(0, NG, start_t, 0)
    m_copy = pltpu.make_async_copy(m_hbm, mv, misc_sem.at[1])
    m_copy.start()

    w_copy.wait()
    wide[...] = jnp.zeros_like(wide)
    wf = wi[...].astype(F32)
    wide[:, 0:FEAT] = wf
    half = ROWS // 2
    wtmp[2 * ROWS : 32, :] = jnp.zeros((32 - 2 * ROWS, 128), F32)
    wtmp[0:ROWS, :] = wide[:, 0:128]
    wtmp[ROWS : 2 * ROWS, :] = wide[:, 128:256]
    wtmp[2 * ROWS : 2 * ROWS + half, :] = wide[0:half, 256:384] + pltpu.roll(
        wide[half:ROWS, 256:384], 64, 1
    )
    wg[core, chip] = wtmp[...].astype(BF16)

    pl.semaphore_wait(barrier, (NCHIP - 1) * NC + NX)

    def w_dst(n):
        return pltpu.make_async_remote_copy(
            src_ref=wg.at[core, chip],
            dst_ref=wg.at[core, chip],
            send_sem=w_send,
            recv_sem=w_recv,
            device_id=(n * NC + core, mx),
            device_id_type=MESH,
        )

    for dy, dz in OFFSETS:
        w_dst(chip_at(dy, dz)).start()

    b_copy.wait()
    wsq[...] = jnp.zeros_like(wsq)
    b_all = bi[...].reshape(1, FEAT)
    b_high = b_all.astype(BF16).astype(F32)
    b_mid = (b_all - b_high).astype(BF16).astype(F32)
    wsq[E : E + 1, 0:FEAT] = b_high
    wsq[E + 1 : E + 2, 0:FEAT] = b_mid
    wsq[E + 2 : E + 3, 0:FEAT] = (b_all - b_high) - b_mid
    acc[...] = jnp.zeros_like(acc)
    lacc[...] = jnp.zeros_like(lacc)
    sc[...] = jnp.zeros_like(sc)
    none = jnp.zeros((RB, 256), BF16)
    for q in range(2):
        pltpu.matmul_acc_lhs(pieces[0], none, load_staged_rhs=q)
        pltpu.matmul_acc_lhs(grad[0], jnp.zeros((FEAT, 256), BF16), load_staged_rhs=q)
    for piece in (*pieces, *grad):
        pltpu.matmul_pop(piece)


    lane_x = lax.broadcasted_iota(jnp.int32, (1, 1, XW - E), 2)
    ones = jnp.where(lane_x < 3, 1.0, 0.0).astype(BF16)

    def stats(g):
        t_copy(g).wait()
        x_copy(g).start()
        xv[pl.ds(g * GI, GI), :, E:XW] = jnp.broadcast_to(ones, (GI, PAT, XW - E))
        sums, squares = [], []
        for k in range(GI):
            s8 = jnp.zeros((8, PAT), F32)
            q8 = jnp.zeros((8, PAT), F32)
            for r in range(0, FEAT, RB):
                t = tv[g * GI + k, r : r + RB, :].astype(F32).reshape(RB // 8, 8, PAT)
                s8 = s8 + jnp.sum(t, axis=0)
                q8 = q8 + jnp.sum(t * t, axis=0)
            sums.append(jnp.sum(s8, axis=0, keepdims=True))
            squares.append(jnp.sum(q8, axis=0, keepdims=True))
        st_own[g] = jnp.concatenate(sums + squares, axis=0)

    def st_copy(g, p):
        return pltpu.make_async_remote_copy(
            src_ref=st_own.at[g],
            dst_ref=st_in.at[p - 1, g],
            send_sem=st_send.at[p - 1, g],
            recv_sem=st_recv.at[p - 1, g],
            device_id=(me, lax.rem(mx + p, NX)),
            device_id_type=MESH,
        )

    def send_stats(g):
        for p in (2, 1, 3):
            st_copy(g, p).start()

    stats(0)

    def stats_and_send(g, _):
        stats(g)
        send_stats(g - 1)
        return 0

    lax.fori_loop(1, NG, stats_and_send, 0)

    m_copy.wait()

    def cover(i, total):
        v = jnp.sum(mv[i].astype(F32), axis=0, keepdims=True)
        vb[i] = jnp.broadcast_to(v, (8, PAT))
        return total + v

    counts = lax.fori_loop(0, IMG, cover, jnp.zeros((1, PAT), F32))
    send_stats(NG - 1)

    def prepare(g):
        for p in (1, 2, 3):
            st_copy(g, p).wait_recv()
        st = (st_own[g] + st_in[0, g]) + (st_in[1, g] + st_in[2, g])
        mean = st[0:GI] * (1.0 / FULL)
        var = jnp.maximum(st[GI : 2 * GI] * (1.0 / FULL) - mean * mean, 0.0)
        a = lax.rsqrt(var + 1e-05)
        c = mean * a
        for k in range(GI):
            ab[g * GI + k] = jnp.broadcast_to(a[k : k + 1], (8, PAT))
            cb[g * GI + k] = jnp.broadcast_to(c[k : k + 1], (8, PAT))

    whole = wg.at[0, pl.ds(0, NCHIP - 1)]
    pltpu.make_async_copy(whole, whole, w_recv).wait()
    w_pair = pltpu.make_async_remote_copy(
        src_ref=wg.at[core], dst_ref=wg.at[core], send_sem=wp_send, recv_sem=wp_recv,
        device_id=(partner, mx), device_id_type=MESH,
    )
    w_pair.start()

    def prepare_all(g, _):
        prepare(g)
        return 0

    lax.fori_loop(0, NG // 4, prepare_all, 0)

    w_pair.wait_recv()

    left = lax.broadcasted_iota(jnp.int32, (half, 128), 1) < 64
    for j in range(NDP):
        r = j * ROWS
        wf32[j] = wg[j % NC, j // NC].astype(F32)
        wsq[r : r + ROWS, 0:128] = wf32[j, 0:ROWS]
        wsq[r : r + ROWS, 128:256] = wf32[j, ROWS : 2 * ROWS]
        both = wf32[j, 2 * ROWS : 2 * ROWS + half]
        wsq[r : r + half, 256:384] = jnp.where(left, both, 0.0)
        wsq[r + half : r + ROWS, 256:384] = jnp.where(left, pltpu.roll(both, 64, 1), 0.0)
    wt[...] = jnp.transpose(wsq[...])[0:FEAT, :].astype(BF16)

    def first(i, pieces):
        for q in range(2):
            pltpu.matmul_push_rhs(
                xv[i, :, 256 * q : 256 * q + 256], staging_register=q, mxu_index=0, transpose=True
            )
        for q in range(2):
            for n, piece in enumerate(pieces):
                pltpu.matmul_acc_lhs(
                    piece, wt[RB * n : RB * n + RB, 256 * q : 256 * q + 256],
                    load_staged_rhs=q if n == 0 else None,
                )

    def second(i, source):
        for q in range(2):
            pltpu.matmul_push_rhs(
                xv[i, :, 256 * q : 256 * q + 256], staging_register=q, mxu_index=1
            )
        for q in range(2):
            pltpu.matmul_acc_lhs(grad[q], source[...], load_staged_rhs=q)

    def middle(i, pieces, target):
        a = ab[i][None]
        c = cb[i][None]
        v = vb[i][None]
        loss8 = jnp.zeros((8, PAT), F32)
        for n, piece in enumerate(pieces):
            r = RB * n
            p = pltpu.matmul_pop(piece).reshape(RB // 8, 8, PAT)
            t = tv[i, r : r + RB, :].astype(F32).reshape(RB // 8, 8, PAT)
            d = p - (t * a - c)
            h = jnp.minimum(jnp.maximum(d, -1.0), 1.0)
            s = v * h
            loss8 = loss8 + jnp.sum(s * (d - 0.5 * h), axis=0)
            s = s.reshape(RB, PAT)
            target[r : r + RB, :] = s.astype(BF16)
            acc[r : r + RB, E : E + 128] += s[:, 0:128] + s[:, 128:256]
        lacc[...] += loss8

    def x_here(g, _):
        x_copy(g).wait()
        return 0

    lax.fori_loop(0, NG, x_here, 0)
    first(0, sets[0])

    def main(g, _):
        base = g * UNROLL
        for u in range(UNROLL):
            first(jnp.minimum(base + u + 1, IMG - 1), sets[(u + 1) % 2])
            second(jnp.maximum(base + u - 1, 0), outs[(u + 1) % 2])
            middle(base + u, sets[u % 2], outs[u % 2])
        return 0

    trips = IMG // UNROLL
    lax.fori_loop(0, trips // 4, main, 0)
    lax.fori_loop(NG // 4, NG, prepare_all, 0)
    lax.fori_loop(trips // 4, trips, main, 0)
    second(IMG - 1, outs[1])
    acc[0:FEAT, 0:256] = pltpu.matmul_pop(grad[0])
    acc[0:FEAT, 256:E] = pltpu.matmul_pop(grad[1])[:, 0:128]
    for piece in sets[0]:
        pltpu.matmul_pop(piece)

    gt[...] = jnp.transpose(acc[...])
    gb = jnp.sum(gt[E : E + 128, :], axis=0, keepdims=True)
    loss_all = jnp.sum(lacc[...])
    count_all = jnp.sum(counts)
    lane = lax.broadcasted_iota(jnp.int32, (1, 128), 1)
    tail = jnp.where(lane < 64, gb[:, 256:384], jnp.where(lane < 96, loss_all, count_all))
    for j in range(NDP):
        r = j * ROWS
        slot = sb.at[j % NC, j // NC]
        slot[0:ROWS, :] = gt[r : r + ROWS, 0:128]
        slot[ROWS : 2 * ROWS, :] = gt[r : r + ROWS, 128:256]
        half = ROWS // 2
        up = gt[r : r + half, 256:384]
        down = gt[r + half : r + ROWS, 256:384]
        slot[2 * ROWS : 2 * ROWS + half, :] = up + pltpu.roll(down, 64, 1)
        slot[30:31, :] = gb[:, 0:128]
        slot[31:32, :] = gb[:, 128:256]
        slot[32:33, :] = tail

    order = [chip_at(dy, dz) for dy, dz in OFFSETS] + [chip]

    def pair(k):
        n = order[k]
        return pltpu.make_async_remote_copy(
            src_ref=sb.at[1 - core, n, pl.ds(0, SLOT)], dst_ref=pin.at[n, pl.ds(0, SLOT)],
            send_sem=c_send.at[k], recv_sem=c_recv.at[k],
            device_id=(partner, mx), device_id_type=MESH,
        )

    def r_copy(n):
        return pltpu.make_async_remote_copy(
            src_ref=ps.at[n, pl.ds(0, SLOT)], dst_ref=rr.at[chip, pl.ds(0, SLOT)],
            send_sem=r_send, recv_sem=r_recv,
            device_id=(n * NC + core, mx), device_id_type=MESH,
        )

    for k in range(NCHIP):
        pair(k).start()
    for k in range(NCHIP):
        n = order[k]
        pair(k).wait_recv()
        both = sb[core, n, 0:SLOT] + pin[n, 0:SLOT]
        if k < NCHIP - 1:
            ps[n, 0:SLOT] = both
        else:
            rr[n, 0:SLOT] = both
        if k > 0:
            r_copy(order[k - 1]).start()
    others = rr.at[pl.ds(0, NCHIP - 1), pl.ds(0, SLOT)]
    pltpu.make_async_copy(others, others, r_recv).wait()
    mine = jnp.sum(rr[:, 0:SLOT], axis=0)
    gbl = mine[30:33]
    lane3 = lax.broadcasted_iota(jnp.int32, (3, 128), 1)
    row3 = lax.broadcasted_iota(jnp.int32, (3, 128), 0)
    gbz = jnp.where((row3 < 2) | (lane3 < 64), gbl, 0.0)
    squares = jnp.sum(mine[0:30] * mine[0:30], axis=0, keepdims=True) + jnp.sum(
        gbz * gbz, axis=0, keepdims=True
    ) * (1.0 / NDP)
    lrow = mine[32:33, :]
    ident = me * NX + mx
    nb[ident] = jnp.where(lane < 64, squares + pltpu.roll(squares, 64, 1), lrow)

    def b_out(n, m):
        return pltpu.make_async_remote_copy(
            src_ref=nb.at[ident], dst_ref=nb.at[ident], send_sem=b_send, recv_sem=b_recv,
            device_id=(n, m), device_id_type=MESH,
        )

    for dx, dy, dz in EVERY:
        for c in range(NC):
            b_out(chip_at(dy, dz) * NC + c, lax.rem(mx + dx, NX)).start()
    b_out(partner, mx).start()
    rest_b = nb.at[pl.ds(0, NDP * NX - 1)]
    def drain(g, _):
        for p in (1, 2, 3):
            st_copy(g, p).wait_send()
        return 0

    lax.fori_loop(0, NG, drain, 0)
    pltpu.make_async_copy(whole, whole, w_send).wait()
    w_pair.wait_send()
    for k in range(NCHIP):
        pair(k).wait_send()
    sent = ps.at[pl.ds(0, NCHIP - 1), pl.ds(0, SLOT)]
    pltpu.make_async_copy(sent, sent, r_send).wait()
    pltpu.make_async_copy(rest_b, rest_b, b_recv).wait()
    parts = [jnp.sum(nb[16 * q : 16 * q + 16], axis=0) for q in range(NDP * NX // 16)]
    final = ((parts[0] + parts[1]) + (parts[2] + parts[3])) + (
        (parts[4] + parts[5]) + (parts[6] + parts[7])
    )
    loss_sum = jnp.sum(jnp.where(lane == 64, final, 0.0)) * (1.0 / NDP)
    count = jnp.sum(jnp.where(lane == 96, lrow, 0.0))
    total = jnp.full((1, 128), jnp.sum(jnp.where(lane < 64, final, 0.0)), F32)
    countv = jnp.full((1, 128), count, F32)
    norm = jnp.sqrt(total) / countv
    clip = jnp.minimum(1.0, 1.0 / (norm + 1e-06))
    factor = clip / countv
    loss = jnp.full((1, 128), loss_sum, F32) / countv * (1.0 / FULL)
    out_o[0:SLOT] = mine * factor
    out_o[SLOT : SLOT + 1] = loss
    out_o[SLOT + 1 : SLOT + 2] = clip
    out_o[SLOT + 2 :] = jnp.zeros((40 - SLOT - 2, 128), F32)
    pltpu.make_async_copy(rest_b, rest_b, b_send).wait()


def spread(in_ref, loss_o, clip_o, gw_o, gb_o):
    half = ROWS // 2
    gw_o[:, 0:128] = in_ref[0:ROWS]
    gw_o[:, 128:256] = in_ref[ROWS : 2 * ROWS]
    gw_o[0:half, 256:320] = in_ref[2 * ROWS : 2 * ROWS + half, 0:64]
    gw_o[half:ROWS, 256:320] = in_ref[2 * ROWS : 2 * ROWS + half, 64:128]
    gb_o[...] = jnp.concatenate(
        [in_ref[30:31, :], in_ref[31:32, :], in_ref[32:33, 0:64]], axis=1
    ).reshape(FEAT)
    loss_o[...] = in_ref[33:34, 0:1]
    clip_o[...] = in_ref[34:35, 0:1]


def body(pred_input, proj_weight, proj_bias, targets, block_masks):
    any_spec = pl.BlockSpec(memory_space=pl.ANY)
    vmem_spec = pl.BlockSpec(memory_space=pltpu.VMEM)
    vm = pltpu.VMEM
    dma = pltpu.SemaphoreType.DMA
    packed = pl.pallas_call(
        kernel,
        name="fused",
        out_shape=jax.ShapeDtypeStruct((40, 128), F32),
        in_specs=[any_spec] * 5,
        out_specs=vmem_spec,
        scratch_shapes=[
            vm((IMG, PAT, XW), BF16),
            vm((IMG, FEAT, PAT), BF16),
            vm((IMG, 4, PAT), jnp.int32),
            vm((ROWS, FEAT), BF16),
            vm((32, 128), F32),
            vm((NDP, 32, 128), F32),
            vm((NC, NCHIP, 32, 128), BF16),
            vm((XW, FP), F32),
            vm((FEAT, XW), BF16),
            vm((FEAT,), F32),
            vm((ROWS, FP), F32),
            vm((NG, 2 * GI, PAT), F32),
            vm((NX - 1, NG, 2 * GI, PAT), F32),
            vm((IMG, 8, PAT), F32),
            vm((IMG, 8, PAT), F32),
            vm((IMG, 8, PAT), F32),
            vm((FEAT, PAT), BF16),
            vm((FEAT, PAT), BF16),
            vm((FP, E + 128), F32),
            vm((8, PAT), F32),
            vm((E + 128, FP), F32),
            vm((NC, NCHIP, 40, 128), F32),
            vm((NCHIP, 40, 128), F32),
            vm((NCHIP, 40, 128), F32),
            vm((NCHIP, 40, 128), F32),
            vm((NDP * NX, 1, 128), F32),
            dma((NG,)), dma((NG,)), dma((3,)),
            dma((NX - 1, NG)), dma((NX - 1, NG)),
            dma, dma, dma, dma, dma((NCHIP,)), dma((NCHIP,)), dma, dma, dma, dma,
        ],
        compiler_params=pltpu.CompilerParams(
            collective_id=0, has_side_effects=True, vmem_limit_bytes=64 * 1024 * 1024 - 65536,
        ),
    )(
        pred_input,
        proj_weight,
        proj_bias,
        jnp.swapaxes(targets, 1, 2),
        block_masks,
    )
    loss, clip, gw, gb = pl.pallas_call(
        spread,
        name="spread",
        out_shape=(
            jax.ShapeDtypeStruct((1, 1), F32),
            jax.ShapeDtypeStruct((1, 1), F32),
            jax.ShapeDtypeStruct((ROWS, FEAT), F32),
            jax.ShapeDtypeStruct((FEAT,), F32),
        ),
        in_specs=[vmem_spec],
        out_specs=(vmem_spec,) * 4,
    )(packed)
    return loss.reshape(()), clip.reshape(()), gw, gb


def solution(mesh):
    return jax.shard_map(
        body,
        mesh=mesh,
        in_specs=(
            P("dp", None, None), P("dp", "mp"), P("mp"), P("dp", None, "mp"), P("dp", None, None),
        ),
        out_specs=(P(), P(), P("dp", "mp"), P("mp")),
        check_vma=False,
    )
```

```python
import jax
import jax.numpy as jnp
from jax import lax
from jax.experimental import pallas as pl
from jax.experimental.pallas import tpu as pltpu
from jax.sharding import PartitionSpec as P

MESH = pl.DeviceIdType.MESH
F32 = jnp.float32
BF16 = jnp.bfloat16

NY, NZ, NC, NX = 4, 4, 2, 4
NCHIP = NY * NZ
NDP = NCHIP * NC
GI = 4
NG = 16
IMG = GI * NG
PAT = 256
FEAT = 320
FULL = FEAT * NX
E = 384
ROWS = E // NDP
FP = 384
RB = 64
XW = 512
UNROLL = 16
SLOT = 33

EVERY = sorted(
    [
        (dx, dy, dz)
        for dx in range(NX) for dy in range(NY) for dz in range(NZ)
        if (dx, dy, dz) != (0, 0, 0)
    ],
    key=lambda o: -(min(o[0], NX - o[0]) + min(o[1], NY - o[1]) + min(o[2], NZ - o[2])),
)
OFFSETS = sorted(
    [(dy, dz) for dy in range(NY) for dz in range(NZ) if (dy, dz) != (0, 0)],
    key=lambda o: -(min(o[0], NY - o[0]) + min(o[1], NZ - o[1])),
)


def kernel(*args):
    pl.run_scoped(
        lambda *refs: work(refs[:-2], refs[-2:], *args),
        *([pltpu.ACC(0)((RB, 256), F32)] * (2 * FEAT // RB) + [pltpu.ACC(1)((FEAT, 256), F32)] * 2),
    )


def work(
    pieces, grad,
    x_hbm, w_hbm, b_hbm, t_hbm, m_hbm,
    out_o,
    xv, tv, mv, wi, wtmp, wf32, wg, wsq, wt, bi, wide,
    st_own, st_in, ab, cb, vb, sa, sc, acc, lacc, gt, sb, pin, ps, rr, nb,
    x_sem, t_sem, misc_sem,
    st_send, st_recv, w_send, w_recv, wp_send, wp_recv, c_send, c_recv, r_send, r_recv, b_send, b_recv,
):
    sets = (pieces[: FEAT // RB], pieces[FEAT // RB :])
    outs = (sa, sc)
    me = lax.axis_index("dp")
    mx = lax.axis_index("mp")
    core = lax.rem(me, NC)
    chip = lax.div(me, NC)
    my_y = lax.div(chip, NZ)
    my_z = lax.rem(chip, NZ)
    partner = me + 1 - 2 * core

    def chip_at(dy, dz):
        return lax.rem(my_y + dy, NY) * NZ + lax.rem(my_z + dz, NZ)

    w_copy = pltpu.make_async_copy(w_hbm, wi, misc_sem.at[0])
    w_copy.start()
    b_copy = pltpu.make_async_copy(b_hbm, bi, misc_sem.at[2])
    b_copy.start()

    barrier = pltpu.get_barrier_semaphore()
    for dy, dz in OFFSETS:
        for c in range(NC):
            pl.semaphore_signal(
                barrier, inc=1, device_id=(chip_at(dy, dz) * NC + c, mx), device_id_type=MESH
            )
    pl.semaphore_signal(barrier, inc=1, device_id=(partner, mx), device_id_type=MESH)
    for dx in range(1, NX):
        pl.semaphore_signal(
            barrier, inc=1, device_id=(me, lax.rem(mx + dx, NX)), device_id_type=MESH
        )

    def t_copy(g):
        return pltpu.make_async_copy(
            t_hbm.at[pl.ds(g * GI, GI)], tv.at[pl.ds(g * GI, GI)], t_sem.at[g]
        )

    def x_copy(g):
        return pltpu.make_async_copy(
            x_hbm.at[pl.ds(g * GI, GI)], xv.at[pl.ds(g * GI, GI), :, pl.ds(0, E)], x_sem.at[g]
        )

    def start_t(g, _):
        t_copy(g).start()
        return 0

    lax.fori_loop(0, NG, start_t, 0)
    m_copy = pltpu.make_async_copy(m_hbm, mv, misc_sem.at[1])
    m_copy.start()

    w_copy.wait()
    wide[...] = jnp.zeros_like(wide)
    wf = wi[...].astype(F32)
    wide[:, 0:FEAT] = wf
    half = ROWS // 2
    wtmp[2 * ROWS : 32, :] = jnp.zeros((32 - 2 * ROWS, 128), F32)
    wtmp[0:ROWS, :] = wide[:, 0:128]
    wtmp[ROWS : 2 * ROWS, :] = wide[:, 128:256]
    wtmp[2 * ROWS : 2 * ROWS + half, :] = wide[0:half, 256:384] + pltpu.roll(
        wide[half:ROWS, 256:384], 64, 1
    )
    wg[core, chip] = wtmp[...].astype(BF16)

    b_copy.wait()
    wsq[...] = jnp.zeros_like(wsq)
    b_all = bi[...].reshape(1, FEAT)
    b_high = b_all.astype(BF16).astype(F32)
    b_mid = (b_all - b_high).astype(BF16).astype(F32)
    wsq[E : E + 1, 0:FEAT] = b_high
    wsq[E + 1 : E + 2, 0:FEAT] = b_mid
    wsq[E + 2 : E + 3, 0:FEAT] = (b_all - b_high) - b_mid
    acc[...] = jnp.zeros_like(acc)
    lacc[...] = jnp.zeros_like(lacc)
    sc[...] = jnp.zeros_like(sc)
    none = jnp.zeros((RB, 256), BF16)
    for q in range(2):
        pltpu.matmul_acc_lhs(pieces[0], none, load_staged_rhs=q)
        pltpu.matmul_acc_lhs(grad[0], jnp.zeros((FEAT, 256), BF16), load_staged_rhs=q)
    for piece in (*pieces, *grad):
        pltpu.matmul_pop(piece)


    pl.semaphore_wait(barrier, (NCHIP - 1) * NC + NX)

    def w_dst(n):
        return pltpu.make_async_remote_copy(
            src_ref=wg.at[core, chip],
            dst_ref=wg.at[core, chip],
            send_sem=w_send,
            recv_sem=w_recv,
            device_id=(n * NC + core, mx),
            device_id_type=MESH,
        )

    for dy, dz in OFFSETS:
        w_dst(chip_at(dy, dz)).start()

    lane_x = lax.broadcasted_iota(jnp.int32, (1, 1, XW - E), 2)
    ones = jnp.where(lane_x < 3, 1.0, 0.0).astype(BF16)

    def stats(g):
        t_copy(g).wait()
        x_copy(g).start()
        xv[pl.ds(g * GI, GI), :, E:XW] = jnp.broadcast_to(ones, (GI, PAT, XW - E))
        sums, squares = [], []
        for k in range(GI):
            s8 = jnp.zeros((8, PAT), F32)
            q8 = jnp.zeros((8, PAT), F32)
            for r in range(0, FEAT, RB):
                t = tv[g * GI + k, r : r + RB, :].astype(F32).reshape(RB // 8, 8, PAT)
                s8 = s8 + jnp.sum(t, axis=0)
                q8 = q8 + jnp.sum(t * t, axis=0)
            sums.append(jnp.sum(s8, axis=0, keepdims=True))
            squares.append(jnp.sum(q8, axis=0, keepdims=True))
        st_own[g] = jnp.concatenate(sums + squares, axis=0)

    def st_copy(g, p):
        return pltpu.make_async_remote_copy(
            src_ref=st_own.at[g],
            dst_ref=st_in.at[p - 1, g],
            send_sem=st_send.at[p - 1, g],
            recv_sem=st_recv.at[p - 1, g],
            device_id=(me, lax.rem(mx + p, NX)),
            device_id_type=MESH,
        )

    def send_stats(g):
        for p in (2, 1, 3):
            st_copy(g, p).start()

    stats(0)

    def stats_and_send(g, _):
        stats(g)
        send_stats(g - 1)
        return 0

    lax.fori_loop(1, NG, stats_and_send, 0)

    m_copy.wait()

    def cover(i, total):
        v = jnp.sum(mv[i].astype(F32), axis=0, keepdims=True)
        vb[i] = jnp.broadcast_to(v, (8, PAT))
        return total + v

    counts = lax.fori_loop(0, IMG, cover, jnp.zeros((1, PAT), F32))
    send_stats(NG - 1)

    def prepare(g):
        for p in (1, 2, 3):
            st_copy(g, p).wait_recv()
        st = (st_own[g] + st_in[0, g]) + (st_in[1, g] + st_in[2, g])
        mean = st[0:GI] * (1.0 / FULL)
        var = jnp.maximum(st[GI : 2 * GI] * (1.0 / FULL) - mean * mean, 0.0)
        a = lax.rsqrt(var + 1e-05)
        c = mean * a
        for k in range(GI):
            ab[g * GI + k] = jnp.broadcast_to(a[k : k + 1], (8, PAT))
            cb[g * GI + k] = jnp.broadcast_to(c[k : k + 1], (8, PAT))

    whole = wg.at[0, pl.ds(0, NCHIP - 1)]
    pltpu.make_async_copy(whole, whole, w_recv).wait()
    w_pair = pltpu.make_async_remote_copy(
        src_ref=wg.at[core], dst_ref=wg.at[core], send_sem=wp_send, recv_sem=wp_recv,
        device_id=(partner, mx), device_id_type=MESH,
    )
    w_pair.start()

    def prepare_all(g, _):
        prepare(g)
        return 0

    lax.fori_loop(0, NG // 4, prepare_all, 0)

    w_pair.wait_recv()

    left = lax.broadcasted_iota(jnp.int32, (half, 128), 1) < 64
    for j in range(NDP):
        r = j * ROWS
        wf32[j] = wg[j % NC, j // NC].astype(F32)
        wsq[r : r + ROWS, 0:128] = wf32[j, 0:ROWS]
        wsq[r : r + ROWS, 128:256] = wf32[j, ROWS : 2 * ROWS]
        both = wf32[j, 2 * ROWS : 2 * ROWS + half]
        wsq[r : r + half, 256:384] = jnp.where(left, both, 0.0)
        wsq[r + half : r + ROWS, 256:384] = jnp.where(left, pltpu.roll(both, 64, 1), 0.0)
    wt[...] = jnp.transpose(wsq[...])[0:FEAT, :].astype(BF16)

    def first(i, pieces):
        for q in range(2):
            pltpu.matmul_push_rhs(
                xv[i, :, 256 * q : 256 * q + 256], staging_register=q, mxu_index=0, transpose=True
            )
        for q in range(2):
            for n, piece in enumerate(pieces):
                pltpu.matmul_acc_lhs(
                    piece, wt[RB * n : RB * n + RB, 256 * q : 256 * q + 256],
                    load_staged_rhs=q if n == 0 else None,
                )

    def second(i, source):
        for q in range(2):
            pltpu.matmul_push_rhs(
                xv[i, :, 256 * q : 256 * q + 256], staging_register=q, mxu_index=1
            )
        for q in range(2):
            pltpu.matmul_acc_lhs(grad[q], source[...], load_staged_rhs=q)

    def middle(i, pieces, target):
        a = ab[i][None]
        c = cb[i][None]
        v = vb[i][None]
        loss8 = jnp.zeros((8, PAT), F32)
        for n, piece in enumerate(pieces):
            r = RB * n
            p = pltpu.matmul_pop(piece).reshape(RB // 8, 8, PAT)
            t = tv[i, r : r + RB, :].astype(F32).reshape(RB // 8, 8, PAT)
            d = p - (t * a - c)
            h = jnp.minimum(jnp.maximum(d, -1.0), 1.0)
            s = v * h
            loss8 = loss8 + jnp.sum(s * (d - 0.5 * h), axis=0)
            s = s.reshape(RB, PAT)
            target[r : r + RB, :] = s.astype(BF16)
            acc[r : r + RB, E : E + 128] += s[:, 0:128] + s[:, 128:256]
        lacc[...] += loss8

    def x_here(g, _):
        x_copy(g).wait()
        return 0

    lax.fori_loop(0, NG, x_here, 0)
    first(0, sets[0])

    def main(g, _):
        base = g * UNROLL
        for u in range(UNROLL):
            first(jnp.minimum(base + u + 1, IMG - 1), sets[(u + 1) % 2])
            second(jnp.maximum(base + u - 1, 0), outs[(u + 1) % 2])
            middle(base + u, sets[u % 2], outs[u % 2])
        return 0

    trips = IMG // UNROLL
    lax.fori_loop(0, trips // 4, main, 0)
    lax.fori_loop(NG // 4, NG, prepare_all, 0)
    lax.fori_loop(trips // 4, trips, main, 0)
    second(IMG - 1, outs[1])
    acc[0:FEAT, 0:256] = pltpu.matmul_pop(grad[0])
    acc[0:FEAT, 256:E] = pltpu.matmul_pop(grad[1])[:, 0:128]
    for piece in sets[0]:
        pltpu.matmul_pop(piece)

    gt[...] = jnp.transpose(acc[...])
    gb = jnp.sum(gt[E : E + 128, :], axis=0, keepdims=True)
    loss_all = jnp.sum(lacc[...])
    count_all = jnp.sum(counts)
    lane = lax.broadcasted_iota(jnp.int32, (1, 128), 1)
    tail = jnp.where(lane < 64, gb[:, 256:384], jnp.where(lane < 96, loss_all, count_all))
    for j in range(NDP):
        r = j * ROWS
        slot = sb.at[j % NC, j // NC]
        slot[0:ROWS, :] = gt[r : r + ROWS, 0:128]
        slot[ROWS : 2 * ROWS, :] = gt[r : r + ROWS, 128:256]
        half = ROWS // 2
        up = gt[r : r + half, 256:384]
        down = gt[r + half : r + ROWS, 256:384]
        slot[2 * ROWS : 2 * ROWS + half, :] = up + pltpu.roll(down, 64, 1)
        slot[30:31, :] = gb[:, 0:128]
        slot[31:32, :] = gb[:, 128:256]
        slot[32:33, :] = tail

    order = [chip_at(dy, dz) for dy, dz in OFFSETS] + [chip]

    def pair(k):
        n = order[k]
        return pltpu.make_async_remote_copy(
            src_ref=sb.at[1 - core, n, pl.ds(0, SLOT)], dst_ref=pin.at[n, pl.ds(0, SLOT)],
            send_sem=c_send.at[k], recv_sem=c_recv.at[k],
            device_id=(partner, mx), device_id_type=MESH,
        )

    def r_copy(n):
        return pltpu.make_async_remote_copy(
            src_ref=ps.at[n, pl.ds(0, SLOT)], dst_ref=rr.at[chip, pl.ds(0, SLOT)],
            send_sem=r_send, recv_sem=r_recv,
            device_id=(n * NC + core, mx), device_id_type=MESH,
        )

    for k in range(NCHIP):
        pair(k).start()
    for k in range(NCHIP):
        n = order[k]
        pair(k).wait_recv()
        both = sb[core, n, 0:SLOT] + pin[n, 0:SLOT]
        if k < NCHIP - 1:
            ps[n, 0:SLOT] = both
        else:
            rr[n, 0:SLOT] = both
        if k > 0:
            r_copy(order[k - 1]).start()
    others = rr.at[pl.ds(0, NCHIP - 1), pl.ds(0, SLOT)]
    pltpu.make_async_copy(others, others, r_recv).wait()
    mine = jnp.sum(rr[:, 0:SLOT], axis=0)
    gbl = mine[30:33]
    lane3 = lax.broadcasted_iota(jnp.int32, (3, 128), 1)
    row3 = lax.broadcasted_iota(jnp.int32, (3, 128), 0)
    gbz = jnp.where((row3 < 2) | (lane3 < 64), gbl, 0.0)
    squares = jnp.sum(mine[0:30] * mine[0:30], axis=0, keepdims=True) + jnp.sum(
        gbz * gbz, axis=0, keepdims=True
    ) * (1.0 / NDP)
    lrow = mine[32:33, :]
    ident = me * NX + mx
    nb[ident] = jnp.where(lane < 64, squares + pltpu.roll(squares, 64, 1), lrow)

    def b_out(n, m):
        return pltpu.make_async_remote_copy(
            src_ref=nb.at[ident], dst_ref=nb.at[ident], send_sem=b_send, recv_sem=b_recv,
            device_id=(n, m), device_id_type=MESH,
        )

    for dx, dy, dz in EVERY:
        for c in range(NC):
            b_out(chip_at(dy, dz) * NC + c, lax.rem(mx + dx, NX)).start()
    b_out(partner, mx).start()
    rest_b = nb.at[pl.ds(0, NDP * NX - 1)]
    def drain(g, _):
        for p in (1, 2, 3):
            st_copy(g, p).wait_send()
        return 0

    lax.fori_loop(0, NG, drain, 0)
    pltpu.make_async_copy(whole, whole, w_send).wait()
    w_pair.wait_send()
    for k in range(NCHIP):
        pair(k).wait_send()
    sent = ps.at[pl.ds(0, NCHIP - 1), pl.ds(0, SLOT)]
    pltpu.make_async_copy(sent, sent, r_send).wait()
    pltpu.make_async_copy(rest_b, rest_b, b_recv).wait()
    parts = [jnp.sum(nb[16 * q : 16 * q + 16], axis=0) for q in range(NDP * NX // 16)]
    final = ((parts[0] + parts[1]) + (parts[2] + parts[3])) + (
        (parts[4] + parts[5]) + (parts[6] + parts[7])
    )
    loss_sum = jnp.sum(jnp.where(lane == 64, final, 0.0)) * (1.0 / NDP)
    count = jnp.sum(jnp.where(lane == 96, lrow, 0.0))
    total = jnp.full((1, 128), jnp.sum(jnp.where(lane < 64, final, 0.0)), F32)
    countv = jnp.full((1, 128), count, F32)
    norm = jnp.sqrt(total) / countv
    clip = jnp.minimum(1.0, 1.0 / (norm + 1e-06))
    factor = clip / countv
    loss = jnp.full((1, 128), loss_sum, F32) / countv * (1.0 / FULL)
    out_o[0:SLOT] = mine * factor
    out_o[SLOT : SLOT + 1] = loss
    out_o[SLOT + 1 : SLOT + 2] = clip
    out_o[SLOT + 2 :] = jnp.zeros((40 - SLOT - 2, 128), F32)
    pltpu.make_async_copy(rest_b, rest_b, b_send).wait()


def spread(in_ref, loss_o, clip_o, gw_o, gb_o):
    half = ROWS // 2
    gw_o[:, 0:128] = in_ref[0:ROWS]
    gw_o[:, 128:256] = in_ref[ROWS : 2 * ROWS]
    gw_o[0:half, 256:320] = in_ref[2 * ROWS : 2 * ROWS + half, 0:64]
    gw_o[half:ROWS, 256:320] = in_ref[2 * ROWS : 2 * ROWS + half, 64:128]
    gb_o[...] = jnp.concatenate(
        [in_ref[30:31, :], in_ref[31:32, :], in_ref[32:33, 0:64]], axis=1
    ).reshape(FEAT)
    loss_o[...] = in_ref[33:34, 0:1]
    clip_o[...] = in_ref[34:35, 0:1]


def body(pred_input, proj_weight, proj_bias, targets, block_masks):
    any_spec = pl.BlockSpec(memory_space=pl.ANY)
    vmem_spec = pl.BlockSpec(memory_space=pltpu.VMEM)
    vm = pltpu.VMEM
    dma = pltpu.SemaphoreType.DMA
    packed = pl.pallas_call(
        kernel,
        name="fused",
        out_shape=jax.ShapeDtypeStruct((40, 128), F32),
        in_specs=[any_spec] * 5,
        out_specs=vmem_spec,
        scratch_shapes=[
            vm((IMG, PAT, XW), BF16),
            vm((IMG, FEAT, PAT), BF16),
            vm((IMG, 4, PAT), jnp.int32),
            vm((ROWS, FEAT), BF16),
            vm((32, 128), F32),
            vm((NDP, 32, 128), F32),
            vm((NC, NCHIP, 32, 128), BF16),
            vm((XW, FP), F32),
            vm((FEAT, XW), BF16),
            vm((FEAT,), F32),
            vm((ROWS, FP), F32),
            vm((NG, 2 * GI, PAT), F32),
            vm((NX - 1, NG, 2 * GI, PAT), F32),
            vm((IMG, 8, PAT), F32),
            vm((IMG, 8, PAT), F32),
            vm((IMG, 8, PAT), F32),
            vm((FEAT, PAT), BF16),
            vm((FEAT, PAT), BF16),
            vm((FP, E + 128), F32),
            vm((8, PAT), F32),
            vm((E + 128, FP), F32),
            vm((NC, NCHIP, 40, 128), F32),
            vm((NCHIP, 40, 128), F32),
            vm((NCHIP, 40, 128), F32),
            vm((NCHIP, 40, 128), F32),
            vm((NDP * NX, 1, 128), F32),
            dma((NG,)), dma((NG,)), dma((3,)),
            dma((NX - 1, NG)), dma((NX - 1, NG)),
            dma, dma, dma, dma, dma((NCHIP,)), dma((NCHIP,)), dma, dma, dma, dma,
        ],
        compiler_params=pltpu.CompilerParams(
            collective_id=0, has_side_effects=True, vmem_limit_bytes=64 * 1024 * 1024 - 65536,
        ),
    )(
        pred_input,
        proj_weight,
        proj_bias,
        jnp.swapaxes(targets, 1, 2),
        block_masks,
    )
    loss, clip, gw, gb = pl.pallas_call(
        spread,
        name="spread",
        out_shape=(
            jax.ShapeDtypeStruct((1, 1), F32),
            jax.ShapeDtypeStruct((1, 1), F32),
            jax.ShapeDtypeStruct((ROWS, FEAT), F32),
            jax.ShapeDtypeStruct((FEAT,), F32),
        ),
        in_specs=[vmem_spec],
        out_specs=(vmem_spec,) * 4,
    )(packed)
    return loss.reshape(()), clip.reshape(()), gw, gb


def solution(mesh):
    return jax.shard_map(
        body,
        mesh=mesh,
        in_specs=(
            P("dp", None, None), P("dp", "mp"), P("mp"), P("dp", None, "mp"), P("dp", None, None),
        ),
        out_specs=(P(), P(), P("dp", "mp"), P("mp")),
        check_vma=False,
    )
```
